256 devices in a mesh: dp: 16 (over x, y), mp: 16 (over z, core).
Axes of the slice: x: 4, y: 4, z: 8, core: 2. Of those that a mesh axis runs over, the one named last changes fastest.
Arguments:
- hidden_in: bfloat16 [2048, 4096], P('dp', 'mp'), may hold values from -6 to 6
- lengths: int32 [16], P('dp'), may hold values from 1 to 128
- norm_attn: float32 [4096], replicated, may hold values from 0.25 to 1.75
- q_weight: bfloat16 [4096, 4096], P('dp', 'mp'), may hold values from -0.01171875 to 0.01171875
- k_weight: bfloat16 [4096, 4096], P('dp', 'mp'), may hold values from -0.09375 to 0.09375
- v_weight: bfloat16 [4096, 4096], P('dp', 'mp'), may hold values from -0.09375 to 0.09375
- out_weight_t: bfloat16 [4096, 4096], P('dp', 'mp'), may hold values from -0.09375 to 0.09375
- norm_ffn: float32 [4096], replicated, may hold values from 0.25 to 1.75
- gate_weight: bfloat16 [4096, 10240], P('dp', 'mp'), may hold values from -0.09375 to 0.09375
- up_weight: bfloat16 [4096, 10240], P('dp', 'mp'), may hold values from -0.09375 to 0.09375
- down_weight_t: bfloat16 [4096, 10240], P('dp', 'mp'), may hold values from -0.0625 to 0.0625
- scale_key: float32 [4096], P('mp'), may hold values from 0.25 to 4
- scale_value: float32 [4096], P('mp'), may hold values from 0.1 to 1.9
- scale_ffn: float32 [10240], P('mp'), may hold values from 0.1 to 1.9
- out_grad: bfloat16 [2048, 4096], P('dp'), may hold values from -6 to 6
- position_bias: float32 [64, 128, 128], P('mp'), may hold values from -6 to 256
Outputs:
- block_out: bfloat16 [2048, 4096], P('dp', 'mp')
- input_grad: bfloat16 [2048, 4096], P('dp', 'mp')
- grad_key: float32 [4096], P('mp')
- grad_value: float32 [4096], P('mp')
- grad_ffn: float32 [10240], P('mp')
The draws below stay inside these ranges and needn't reach their ends.
Inputs may be any that keep to these rules, and one draw needn't show every extreme that they name: Keys of sequence b at positions lengths[b] and beyond are padding.
All inputs are finite; a program needn't handle non-finite values.
Results may differ from the reference program's by a relative error of at most 0.03.
Values may be sent and summed in bfloat16 or wider, within the bound.
A program may use at most 128 MiB of HBM per device.

```python
import math
import jax
import jax.numpy as jnp
from jax import lax

D = 4096
FF = 10240
HEADS = 64
HEAD_DIM = 64
SEQ = 128
HD = 4096
BATCH = 16
TOKENS = 2048
N_MP = 16


def draw_position_bias(key, part):
    first_key = jax.random.fold_in(key, 0)
    return jnp.clip(jax.random.normal(first_key, (HEADS, SEQ, SEQ), jnp.float32), -6.0, 6.0)


def with_ends(array, own_key, smallest, largest):
    longest = array.shape.index(max(array.shape))
    spots = []
    for shift in (0, 1):
        where = [jax.random.randint(jax.random.fold_in(own_key, axis), (), 0, length) for axis, length in enumerate(array.shape)]
        where[longest] = (where[longest] + shift) % array.shape[longest]
        spots.append(tuple(where))
    return array.at[spots[0]].set(smallest).at[spots[1]].set(largest)


def block_scale(rng, shape, shards, smallest, top_value):
    factor_of, own = 1.0, jax.random.fold_in(rng, 6)
    for dim, blocks in shards:
        draws = jnp.exp(jax.random.uniform(jax.random.fold_in(own, dim), (blocks,), jnp.float32, smallest / len(shards), top_value / len(shards)))
        factor_of = factor_of * jnp.repeat(draws, shape[dim] // blocks).reshape([-1 if axis == dim else 1 for axis in range(len(shape))])
    return factor_of


def gaussian(stream_key, extent, spread, most, cuts=(), held_as=jnp.bfloat16):
    values = jax.random.normal(stream_key, extent, jnp.float32) * spread
    if len(cuts) > 0:
        values = block_scale(stream_key, extent, cuts, -0.22, 0.18) * values
    return jnp.clip(values, min=-most, max=most).astype(held_as)


def setup_inputs(seed: int = 0) -> dict:
    keys = jax.random.split(jax.random.key(seed), 17)
    return {
        "hidden_in": gaussian(keys[0], (TOKENS, D), 1.0, 6.0, ((0, 16), (1, 16))),
        "lengths": with_ends(jax.random.randint(keys[1], (BATCH,), 1, SEQ + 1), jax.random.fold_in(keys[1], 1), 1, SEQ).astype(jnp.int32),
        "norm_attn": jnp.clip(1.0 + 0.15 * jax.random.normal(keys[2], (D,), jnp.float32), 0.25, 1.75),
        "q_weight": gaussian(keys[3], (D, HD), (D * HEAD_DIM) ** -0.5, 0.01171875, ((0, 16), (1, 16))),
        "k_weight": gaussian(keys[4], (D, HD), D ** -0.5, 0.09375, ((0, 16), (1, 16))),
        "v_weight": gaussian(keys[5], (D, HD), D ** -0.5, 0.09375, ((0, 16), (1, 16))),
        "out_weight_t": gaussian(keys[6], (D, HD), HD ** -0.5, 0.09375, ((0, 16), (1, 16))),
        "norm_ffn": jnp.clip(1.0 + 0.15 * jax.random.normal(keys[7], (D,), jnp.float32), 0.25, 1.75),
        "gate_weight": gaussian(keys[8], (D, FF), D ** -0.5, 0.09375, ((0, 16), (1, 16))),
        "up_weight": gaussian(keys[9], (D, FF), D ** -0.5, 0.09375, ((0, 16), (1, 16))),
        "down_weight_t": gaussian(keys[10], (D, FF), FF ** -0.5, 0.0625, ((0, 16), (1, 16))),
        "scale_key": jnp.clip(jnp.exp(math.log(4.0) - 2.7725887 * jax.random.uniform(keys[11], (HD,), jnp.float32) ** block_scale(keys[11], (HD,), ((0, 16),), -0.2, 0.2)), 0.25, 4.0),
        "scale_value": jnp.clip(1.0 + 0.18 * jax.random.normal(keys[12], (HD,), jnp.float32), 0.1, 1.9),
        "scale_ffn": jnp.clip(1.0 + 0.18 * jax.random.normal(keys[13], (FF,), jnp.float32), 0.1, 1.9),
        "out_grad": gaussian(keys[14], (TOKENS, D), 1.0, 6.0, ((0, 16),)),
        "position_bias": draw_position_bias(jax.random.fold_in(keys[16], 71), 0),
    }


EPSILON = 1e-06
NEGATIVE = -1e+30

def inverse_rms(values):
    return lax.rsqrt(lax.optimization_barrier(jnp.mean(values * values, axis=-1, keepdims=True)) + EPSILON)

def lowered(values):
    return lax.optimization_barrier(values.astype(jnp.bfloat16))

def widen(values):
    return values.astype(jnp.float32)

def gelu_tanh(values):
    return jax.nn.gelu(values, approximate=True)

def contract_last(left_side, right_side):
    return lax.dot_general(left_side, right_side, (((1,), (1,)), ((), ())), preferred_element_type=jnp.float32)

def block_split(matrix, block_count):
    return jnp.transpose(matrix.reshape(matrix.shape[0], block_count, -1), (1, 0, 2))

def rounded_blocks(operands, block_count):
    row_count = operands[0][0].shape[0]
    out_width = operands[0][1].shape[0]
    stacked = tuple((block_split(member, block_count) for couple in operands for member in couple))

    def accumulate(running, pieces):
        partial_term = jnp.zeros((row_count, out_width), jnp.float32)
        for position in range(len(operands)):
            partial_term = partial_term + contract_last(pieces[2 * position], pieces[2 * position + 1])
        rounded = lax.optimization_barrier(partial_term.astype(jnp.bfloat16))
        return (running + rounded.astype(jnp.float32), None)
    result, unused = lax.scan(accumulate, jnp.zeros((row_count, out_width), jnp.float32), stacked)
    return result

def norm_back(grad_in, values, inverse, gain_vec):
    scaled = grad_in * gain_vec
    correction = values * inverse * inverse * inverse * lax.optimization_barrier(jnp.mean(scaled * values, axis=-1, keepdims=True))
    return inverse * scaled - correction

def reference(hidden_in, lengths, norm_attn, q_weight, k_weight, v_weight, out_weight_t, norm_ffn, gate_weight, up_weight, down_weight_t, scale_key, scale_value, scale_ffn, out_grad, position_bias):
    shaped = (BATCH, SEQ, HEADS, HEAD_DIM)
    inputs32 = hidden_in.astype(jnp.float32)
    inv_first = inverse_rms(inputs32)
    normed_first = (inputs32 * inv_first * norm_attn).astype(jnp.bfloat16)
    queries = lowered(jnp.dot(normed_first, q_weight, preferred_element_type=jnp.float32))
    key_pre = jnp.dot(normed_first, k_weight, preferred_element_type=jnp.float32)
    value_pre = jnp.dot(normed_first, v_weight, preferred_element_type=jnp.float32)
    key_rows = lowered(key_pre * scale_key)
    value_rows = lowered(value_pre * scale_value)
    q_heads = widen(queries).reshape(shaped)
    k_heads = widen(key_rows).reshape(shaped)
    v_heads = widen(value_rows).reshape(shaped)
    scores = jnp.einsum('bihe,bjhe->bhij', q_heads, k_heads) + position_bias.astype(jnp.float32)[None]
    positions = jnp.arange(SEQ, dtype=jnp.int32)
    valid_keys = positions[None, :] < lengths[:, None]
    scores = jnp.where(valid_keys[:, None, None, :], scores, NEGATIVE)
    attn_probs = jax.nn.softmax(scores, axis=-1)
    probs_low = widen(lowered(attn_probs))
    context = jnp.einsum('bhij,bjhe->bihe', probs_low, v_heads).reshape(TOKENS, HEADS * HEAD_DIM).astype(jnp.bfloat16)
    first_sum = inputs32 + rounded_blocks(((context, out_weight_t),), N_MP)
    inv_second = inverse_rms(first_sum)
    normed_second = (first_sum * inv_second * norm_ffn).astype(jnp.bfloat16)
    gate_proj = jnp.dot(normed_second, gate_weight, preferred_element_type=jnp.float32)
    upward = jnp.dot(normed_second, up_weight, preferred_element_type=jnp.float32)
    activated, gelu_back = jax.vjp(gelu_tanh, gate_proj)
    product = activated * upward
    hidden = (product * scale_ffn).astype(jnp.bfloat16)
    block_out = (first_sum + rounded_blocks(((hidden, down_weight_t),), N_MP)).astype(jnp.bfloat16)
    d_hidden = jnp.dot(out_grad, down_weight_t, preferred_element_type=jnp.float32)
    grad_ffn = lax.optimization_barrier(jnp.sum(d_hidden * product, axis=0))
    d_product = d_hidden * scale_ffn
    d_gate = gelu_back(d_product * upward)[0].astype(jnp.bfloat16)
    d_up = (d_product * activated).astype(jnp.bfloat16)
    d_second = rounded_blocks(((d_gate, gate_weight), (d_up, up_weight)), N_MP)
    d_first = out_grad.astype(jnp.float32) + norm_back(d_second, first_sum, inv_second, norm_ffn)
    d_context = lowered(jnp.dot(d_first.astype(jnp.bfloat16), out_weight_t, preferred_element_type=jnp.float32))
    dc_heads = widen(d_context).reshape(shaped)
    d_probs = jnp.einsum('bihe,bjhe->bhij', dc_heads, v_heads)
    d_scores = widen(lowered(attn_probs * (d_probs - lax.optimization_barrier(jnp.sum(attn_probs * d_probs, axis=-1, keepdims=True)))))
    d_values = jnp.einsum('bhij,bihe->bjhe', probs_low, dc_heads).reshape(TOKENS, HEADS * HEAD_DIM)
    d_keys = jnp.einsum('bhij,bihe->bjhe', d_scores, q_heads).reshape(TOKENS, HEADS * HEAD_DIM)
    d_queries = jnp.einsum('bhij,bjhe->bihe', d_scores, k_heads).reshape(TOKENS, HEADS * HEAD_DIM).astype(jnp.bfloat16)
    grad_key = lax.optimization_barrier(jnp.sum(d_keys * key_pre, axis=0))
    grad_value = lax.optimization_barrier(jnp.sum(d_values * value_pre, axis=0))
    d_key_pre = (d_keys * scale_key).astype(jnp.bfloat16)
    d_value_pre = (d_values * scale_value).astype(jnp.bfloat16)
    d_normed = rounded_blocks(((d_queries, q_weight), (d_key_pre, k_weight), (d_value_pre, v_weight)), N_MP)
    input_grad = (d_first + norm_back(d_normed, inputs32, inv_first, norm_attn)).astype(jnp.bfloat16)
    return (block_out, input_grad, grad_key, grad_value, grad_ffn)
```

```python
import functools
import math

import jax
import jax.numpy as jnp
from jax import lax
from jax.experimental import pallas as pl
from jax.experimental.pallas import tpu as pltpu
from jax.sharding import Mesh
from jax.sharding import PartitionSpec as P

HEAD_DIM = 64
EPSILON = 1e-06
NEGATIVE = -1e30
XA, YA, ZA, CA = "dp_0", "dp_1", "mp_0", "mp_1"
AXES = (XA, YA, ZA, CA)
MESH_ID = pl.DeviceIdType.MESH
F32, BF16 = jnp.float32, jnp.bfloat16
TOK = 128


def far_first(n):
    return sorted(range(1, n), key=lambda d: (-min(d, n - d), d))


def nn(a, b):
    return lax.dot_general(a, b, (((1,), (0,)), ((), ())), preferred_element_type=F32)


def nt(a, b):
    return lax.dot_general(a, b, (((1,), (1,)), ((), ())), preferred_element_type=F32)


def row_sums(values):
    ones = jnp.ones((8, values.shape[1]), BF16)
    return nt(ones, values.astype(BF16))


def as_columns(row, width):
    col = jnp.broadcast_to(row[0:1, :], (TOK, TOK)).T
    return jnp.concatenate([col] * (width // TOK), axis=1)


class Links:
    def __init__(self, sizes, coords, send_sems, recv_sems):
        self.sizes, self.coords = sizes, coords
        self.ss, self.rs = send_sems, recv_sems
        self.used, self.sent = 0, []

    def fresh(self):
        k = self.used
        self.used += 1
        return k

    def copy(self, src, dst, device):
        k = self.fresh()
        return pltpu.make_async_remote_copy(
            src_ref=src,
            dst_ref=dst,
            send_sem=self.ss.at[k],
            recv_sem=self.rs.at[k],
            device_id=device,
            device_id_type=MESH_ID,
        )

    def start(self, src, dst, device):
        copy = self.copy(src, dst, device)
        copy.start()
        self.sent.append(copy)
        return copy

    def peer(self, axis, d):
        return lax.rem(self.coords[axis] + d, self.sizes[axis])

    def share(self, axis, ref, dst=None):
        dst = ref if dst is None else dst
        return {
            d: self.start(ref, dst, {axis: self.peer(axis, d)})
            for d in far_first(self.sizes[axis])
        }

    def local(self, src, dst):
        k = self.fresh()
        copy = pltpu.make_async_copy(src, dst, self.ss.at[k])
        copy.start()
        return copy


def arrived(copies):
    for copy in copies.values() if isinstance(copies, dict) else copies:
        copy.wait_recv()


def layer_kernel(
    sizes,
    x_in,
    og_in,
    wq_in,
    wk_in,
    wv_in,
    wo_in,
    wg_in,
    wu_in,
    wd_in,
    norm_a,
    norm_f,
    par_in,
    len_in,
    bias_in,
    out_ref,
    ig_ref,
    grad_ref,
    wqkv,
    wo,
    wgu,
    wd,
    gx,
    gog,
    gn,
    sq,
    bias_all,
    par_all,
    len_all,
    sb_qkv,
    rb_qkv,
    kv_pre,
    qkv_low,
    probs,
    gctx,
    sb_z,
    rb_z,
    fs_r,
    gfs,
    sb_gu,
    rb_gu,
    sb_dh,
    rb_dh,
    gdgu,
    ghid,
    gdot,
    pz,
    rb_dot,
    df_r,
    gdf,
    sb_dc,
    rb_dc,
    gdqkv,
    gv,
    tout,
    send_sems,
    recv_sems,
):
    nx, ny, nz, nc = sizes
    x, y, z, c = (lax.axis_index(a) for a in AXES)
    seqs = ny // nc
    s_h, hh_h = y // nc, y % nc
    a_r, s_r = z // seqs, z % seqs
    head_cols = wq_in.shape[1]
    ff_cols = wg_in.shape[1]
    rows = wq_in.shape[0]
    width = rows * nx * ny
    links = Links(dict(zip(AXES, sizes)), dict(zip(AXES, (x, y, z, c))), send_sems, recv_sems)

    partner = (x, nc * s_r + c, seqs * a_r + s_h, hh_h)
    at_home = jnp.logical_and(s_h == s_r, hh_h == c)
    away = jnp.logical_not(at_home)

    barrier = pltpu.get_barrier_semaphore()
    greeted = 0
    for axis, n in zip(AXES, sizes):
        for d in range(1, n):
            pl.semaphore_signal(
                barrier, inc=1, device_id={axis: links.peer(axis, d)}, device_id_type=MESH_ID
            )
            greeted += 1

    @pl.when(away)
    def _():
        pl.semaphore_signal(barrier, inc=1, device_id=partner, device_id_type=MESH_ID)
        pl.semaphore_wait(barrier, greeted + 1)

    @pl.when(at_home)
    def _():
        pl.semaphore_wait(barrier, greeted)

    def swapped(src, dst):
        away_copy = links.copy(src, dst, partner)
        k = links.fresh()
        home_copy = pltpu.make_async_copy(src, dst, links.ss.at[k])

        @pl.when(away)
        def _():
            away_copy.start()

        @pl.when(at_home)
        def _():
            home_copy.start()

        def done():
            @pl.when(away)
            def _():
                away_copy.wait()

            @pl.when(at_home)
            def _():
                home_copy.wait()

        return done

    z_there = seqs * a_r + s_h
    own_block = nc * z + c
    x_moved = swapped(x_in, gx.at[z_there])
    og_moved = swapped(
        og_in.at[:, pl.ds(pl.multiple_of(own_block * rows, rows), rows)], gog.at[z_there]
    )

    def w_spot(buf, col, n, there):
        spot = pl.ds(pl.multiple_of(there * rows, rows), rows)
        return buf.at[c, spot, pl.ds(col, n)]

    matrices = (
        ("q", wq_in, wqkv, 0),
        ("k", wk_in, wqkv, head_cols),
        ("v", wv_in, wqkv, 2 * head_cols),
        ("o", wo_in, wo, 0),
        ("d", wd_in, wd, 0),
        ("g", wg_in, wgu, 0),
        ("u", wu_in, wgu, ff_cols),
    )
    over_x, own_w, to_core = {}, {}, {}
    for name, src, buf, col in matrices:
        n = src.shape[1]
        over_x[name] = {
            d: links.start(src, w_spot(buf, col, n, x), {XA: links.peer(XA, d)})
            for d in far_first(nx)
        }
        own_w[name] = links.local(src, w_spot(buf, col, n, x))
        to_core[name] = [
            links.start(src, w_spot(buf, col, n, x), {CA: links.peer(CA, d)}) for d in range(1, nc)
        ]

    def relay(names):
        for name, src, buf, col in matrices:
            if name in names:
                for d, copy in over_x[name].items():
                    copy.wait_recv()
                    there = lax.rem(x + nx - d, nx)
                    spot = w_spot(buf, col, src.shape[1], there)
                    for e in range(1, nc):
                        to_core[name].append(links.start(spot, spot, {CA: links.peer(CA, e)}))

    def weights_ready(names):
        for name in names:
            own_w[name].wait()
            arrived(to_core[name])

    bias_here = links.local(bias_in, bias_all.at[c])
    small = [
        links.start(bias_in, bias_all.at[c], {CA: links.peer(CA, d)}) for d in range(1, nc)
    ]
    small += [links.start(par_in, par_all.at[c], {CA: links.peer(CA, d)}) for d in range(1, nc)]
    small += list(links.share(YA, len_in, len_all.at[y]).values())
    par_all[c] = par_in[...]
    len_all[y] = len_in[...]

    x_moved()
    x_gathered = links.share(ZA, gx.at[z])
    og_moved()
    og_gathered = links.share(ZA, gog.at[z])

    def wide(blocks, s):
        return jnp.concatenate([blocks[seqs * a + s] for a in range(nx)], axis=1)

    def gain(norm, a):
        return norm[ny * a + y]

    def normed(blocks, norm, k):
        for s in range(seqs):
            total = None
            for a in range(nx):
                v = blocks[seqs * a + s].astype(F32)
                gn[seqs * a + s] = (v * gain(norm, a)).astype(BF16)
                part = row_sums(v * v)
                total = part if total is None else total + part
            sq[k, y, s] = total
        return links.share(YA, sq.at[k, y])

    def inverse(k, s):
        total = sq[k, 0, s]
        for there in range(1, ny):
            total = total + sq[k, there, s]
        return lax.rsqrt(total / width + EPSILON)

    def scatter_y(blocks, weights, sent, landed):
        copies = {}
        for d in far_first(ny) + [0]:
            there = links.peer(YA, d) if d else y
            part = nn(wide(blocks, there // nc), weights[there % nc])
            if d == 0:
                return part, copies
            sent[d - 1] = part.astype(BF16)
            copies[d] = links.start(sent.at[d - 1], landed.at[d - 1], {YA: there})

    def total_of(own, landed, n):
        for d in range(n - 1):
            own = own + landed[d].astype(F32)
        return own

    def scatter_z(k, held, weights, extra=None):
        copies = {}
        for d in far_first(nz) + [0]:
            there = links.peer(ZA, d) if d else z
            a, s = there // seqs, there % seqs
            spot = pl.ds(pl.multiple_of(a * rows, rows), rows)
            part = None
            for hh in range(nc):
                term = nt(held[nc * s + hh], weights[hh, spot, :])
                part = term if part is None else part + term
            if d == 0:
                return part, copies
            sb_z[k, d - 1] = part.astype(BF16)
            copies[d] = links.start(sb_z.at[k, d - 1], rb_z.at[k, d - 1], {ZA: there})
            if extra is not None:
                copies[-d] = links.start(pz.at[extra, s], rb_dot.at[extra, d - 1], {ZA: there})

    def chip_sums(k):
        for s in range(seqs):
            total = gdot[k, nc * s]
            for hh in range(1, nc):
                total = total + gdot[k, nc * s + hh]
            pz[k, s] = total

    relay("qkv")
    arrived(x_gathered)
    sq1 = normed(gx, norm_a, 0)
    weights_ready("qkv")
    own, moved = scatter_y(gn, wqkv, sb_qkv, rb_qkv)
    bias_here.wait()
    arrived(small)
    relay("o")
    arrived(sq1)
    arrived(moved)
    inv_first = as_columns(inverse(0, s_h), 3 * head_cols)
    raw = total_of(own, rb_qkv, ny) * inv_first
    par = par_all[hh_h]
    scale_key = par[0:1, 0:head_cols]
    scale_value = par[0:1, head_cols : 2 * head_cols]
    scale_ffn = par[0:1, 2 * head_cols : 2 * head_cols + ff_cols]
    key_pre = raw[:, head_cols : 2 * head_cols]
    value_pre = raw[:, 2 * head_cols :]
    kv_pre[0] = key_pre
    kv_pre[1] = value_pre
    qkv_low[0] = raw[:, :head_cols].astype(BF16)
    qkv_low[1] = (key_pre * scale_key).astype(BF16)
    qkv_low[2] = (value_pre * scale_value).astype(BF16)
    lane = lax.broadcasted_iota(jnp.int32, (TOK, TOK), 1)
    real = lane.astype(F32) < len_all[nc * s_h + c][0:1, :]
    halves = [lane < HEAD_DIM, lane >= HEAD_DIM]
    zero = jnp.zeros((TOK, TOK), F32)

    def half_of(pair, half):
        return jnp.where(halves[half], pair.astype(F32), zero).astype(BF16)

    pairs = head_cols // TOK
    for pair in range(pairs):
        cols = slice(pair * TOK, (pair + 1) * TOK)
        q2, k2, v2 = (qkv_low[i, :, cols] for i in range(3))
        parts = []
        for half in range(2):
            head = 2 * pair + half
            scores = nt(half_of(q2, half), k2) + bias_all[hh_h, head]
            scores = jnp.where(real, scores, NEGATIVE)
            exponent = jnp.exp(scores - jnp.max(scores, axis=1, keepdims=True))
            prob = exponent / jnp.sum(exponent, axis=1, keepdims=True)
            probs[head] = prob
            parts.append(nn(prob.astype(BF16), v2))
        gctx[y, :, cols] = jnp.where(halves[0], parts[0], parts[1]).astype(BF16)
    ctx_gathered = links.share(YA, gctx.at[y])
    weights_ready("o")
    relay("d")
    arrived(ctx_gathered)
    own, moved = scatter_z(0, gctx, wo)
    weights_ready("d")
    arrived(og_gathered)
    own_dh, dh_moved = scatter_y(gog, wd, sb_dh, rb_dh)
    arrived(moved)
    first_sum = gx[z].astype(F32) + total_of(own, rb_z.at[0], nz)
    fs_r[...] = first_sum
    gfs[z] = first_sum.astype(BF16)
    fs_gathered = links.share(ZA, gfs.at[z])

    relay("gu")
    arrived(fs_gathered)
    sq2 = normed(gfs, norm_f, 1)
    weights_ready("gu")
    own, moved = scatter_y(gn, wgu, sb_gu, rb_gu)
    arrived(sq2)
    arrived(dh_moved)
    arrived(moved)
    d_hidden = total_of(own_dh, rb_dh, ny)
    both = total_of(own, rb_gu, ny) * as_columns(inverse(1, s_h), 2 * ff_cols)
    gate, up = both[:, :ff_cols], both[:, ff_cols:]
    root = math.sqrt(2.0 / math.pi)
    squared = gate * gate
    tanh = jnp.tanh(root * (gate + 0.044715 * gate * squared))
    activated = 0.5 * gate * (1.0 + tanh)
    slope = 0.5 * (1.0 + tanh) + 0.5 * gate * (1.0 - tanh * tanh) * (
        root * (1.0 + (3.0 * 0.044715) * squared)
    )
    product = activated * up
    d_product = d_hidden * scale_ffn
    d_gate = (d_product * up * slope).astype(BF16)
    d_up = (d_product * activated).astype(BF16)
    gdgu[y, :, :ff_cols] = d_gate
    gdgu[y, :, ff_cols:] = d_up
    dgu_gathered = links.share(YA, gdgu.at[y])
    gdot[0, y] = row_sums(d_gate.astype(F32) * gate + d_up.astype(F32) * up)
    dot_gathered = links.share(YA, gdot.at[0, y])
    ghid[y] = (product * scale_ffn).astype(BF16)
    hid_gathered = links.share(YA, ghid.at[y])
    grads_at = 2 * head_cols
    gv[0, 0, 0:1, grads_at:] = jnp.sum(d_hidden * product, axis=0, keepdims=True)
    arrived(dot_gathered)
    chip_sums(0)
    arrived(dgu_gathered)
    own, moved = scatter_z(1, gdgu, wgu, 0)
    inv_second = as_columns(inverse(1, s_r), rows)
    arrived(moved)
    dot = total_of(pz[0, s_r], rb_dot.at[0], nz)
    out_grad_r = gog[z].astype(F32)
    scaled = total_of(own, rb_z.at[1], nz) * gain(norm_f, a_r)
    d_first = (
        out_grad_r
        + inv_second * scaled
        - fs_r[...] * (inv_second * inv_second * as_columns(dot / width, rows))
    )
    df_r[...] = d_first
    gdf[z] = d_first.astype(BF16)
    df_gathered = links.share(ZA, gdf.at[z])
    arrived(hid_gathered)
    own_ff, ff_moved = scatter_z(2, ghid, wd)

    arrived(df_gathered)
    own, moved = scatter_y(gdf, wo, sb_dc, rb_dc)
    arrived(moved)
    d_context = total_of(own, rb_dc, ny).astype(BF16)
    for pair in range(pairs):
        cols = slice(pair * TOK, (pair + 1) * TOK)
        q2, k2, v2 = (qkv_low[i, :, cols] for i in range(3))
        dc2 = d_context[:, cols]
        dq, dk, dv = [], [], []
        for half in range(2):
            prob = probs[2 * pair + half]
            d_probs = nt(half_of(dc2, half), v2)
            inner = jnp.sum(prob * d_probs, axis=1, keepdims=True)
            d_scores = prob * (d_probs - inner)
            dq.append(nn(d_scores.astype(BF16), k2))
            dk.append(nn(d_scores.T.astype(BF16), q2))
            dv.append(nn(prob.T.astype(BF16), dc2))
        d_query, d_key, d_value = (jnp.where(halves[0], *two) for two in (dq, dk, dv))
        key2, value2 = kv_pre[0, :, cols], kv_pre[1, :, cols]
        at = pair * TOK
        gv[0, 0, 0:1, at : at + TOK] = jnp.sum(d_key * key2, axis=0, keepdims=True)
        at += head_cols
        gv[0, 0, 0:1, at : at + TOK] = jnp.sum(d_value * value2, axis=0, keepdims=True)
        d_query = d_query.astype(BF16)
        d_key = (d_key * scale_key[:, cols]).astype(BF16)
        d_value = (d_value * scale_value[:, cols]).astype(BF16)
        terms = (
            d_query.astype(F32) * q2.astype(F32)
            + d_key.astype(F32) * key2
            + d_value.astype(F32) * value2
        )
        sums = row_sums(terms)
        dots = sums if pair == 0 else dots + sums
        for i, part in enumerate((d_query, d_key, d_value)):
            gdqkv[y, :, i * head_cols + pair * TOK : i * head_cols + (pair + 1) * TOK] = part
    dqkv_gathered = links.share(YA, gdqkv.at[y])
    gdot[1, y] = dots
    dot_gathered = links.share(YA, gdot.at[1, y])

    gv_c = links.share(CA, gv.at[0, 0], gv.at[0, 1])
    arrived(ff_moved)
    tout[0] = (fs_r[...] + total_of(own_ff, rb_z.at[2], nz)).astype(BF16)
    out_moved = swapped(tout.at[0], tout.at[2])
    arrived(gv_c)
    total = gv[0, 0]
    if nc > 1:
        total = total + gv[0, 1]
    gv[1, y] = total
    gv_y = links.share(YA, gv.at[1, y])
    arrived(dot_gathered)
    chip_sums(1)
    arrived(dqkv_gathered)
    own, moved = scatter_z(3, gdqkv, wqkv, 1)
    arrived(gv_y)
    total = gv[1, c]
    for s in range(1, seqs):
        total = total + gv[1, nc * s + c]
    gv[2, x] = total
    gv_x = links.share(XA, gv.at[2, x])
    inv_first = as_columns(inverse(0, s_r), rows)
    arrived(moved)
    dot = total_of(pz[1, s_r], rb_dot.at[1], nz)
    scaled = total_of(own, rb_z.at[3], nz) * gain(norm_a, a_r)
    tout[1] = (
        df_r[...]
        + inv_first * scaled
        - gx[z].astype(F32) * (inv_first * inv_first * as_columns(dot / width, rows))
    ).astype(BF16)
    ig_moved = swapped(tout.at[1], tout.at[3])
    arrived(gv_x)
    total = gv[2, 0]
    for there in range(1, nx):
        total = total + gv[2, there]
    grad_ref[...] = total
    out_moved()
    out_ref[...] = tout[2]
    ig_moved()
    ig_ref[...] = tout[3]
    for copy in links.sent:
        copy.wait_send()


def on_device(
    sizes,
    hidden_in,
    lengths,
    norm_attn,
    q_weight,
    k_weight,
    v_weight,
    out_weight_t,
    norm_ffn,
    gate_weight,
    up_weight,
    down_weight_t,
    scale_key,
    scale_value,
    scale_ffn,
    out_grad,
    position_bias,
):
    nx, ny, nz, nc = sizes
    seqs = ny // nc
    rows, head_cols = q_weight.shape
    ff_cols = gate_weight.shape[1]
    blocks = nx * ny
    extra = 2 * head_cols + ff_cols
    par = jnp.broadcast_to(jnp.concatenate([scale_key, scale_value, scale_ffn])[None], (8, extra))
    lens = jnp.broadcast_to(lengths.astype(F32)[:, None], (8, TOK))
    heads = head_cols // HEAD_DIM
    wide = rows * nx
    vmem, hbm = pl.BlockSpec(memory_space=pltpu.VMEM), pl.BlockSpec(memory_space=pl.ANY)

    def buf(*shape, dtype=BF16):
        return pltpu.VMEM(shape, dtype)

    scratch = [
        buf(nc, wide, 3 * head_cols),
        buf(nc, wide, head_cols),
        buf(nc, wide, 2 * ff_cols),
        buf(nc, wide, ff_cols),
        buf(nz, TOK, rows),
        buf(nz, TOK, rows),
        buf(nz, TOK, rows),
        buf(2, ny, seqs, 8, TOK, dtype=F32),
        buf(nc, heads, TOK, TOK, dtype=F32),
        buf(nc, 8, extra, dtype=F32),
        buf(ny, 8, TOK, dtype=F32),
        buf(ny - 1, TOK, 3 * head_cols),
        buf(ny - 1, TOK, 3 * head_cols),
        buf(2, TOK, head_cols, dtype=F32),
        buf(3, TOK, head_cols),
        buf(heads, TOK, TOK, dtype=F32),
        buf(ny, TOK, head_cols),
        buf(4, nz - 1, TOK, rows),
        buf(4, nz - 1, TOK, rows),
        buf(TOK, rows, dtype=F32),
        buf(nz, TOK, rows),
        buf(ny - 1, TOK, 2 * ff_cols),
        buf(ny - 1, TOK, 2 * ff_cols),
        buf(ny - 1, TOK, ff_cols),
        buf(ny - 1, TOK, ff_cols),
        buf(ny, TOK, 2 * ff_cols),
        buf(ny, TOK, ff_cols),
        buf(2, ny, 8, TOK, dtype=F32),
        buf(2, seqs, 8, TOK, dtype=F32),
        buf(2, nz - 1, 8, TOK, dtype=F32),
        buf(TOK, rows, dtype=F32),
        buf(nz, TOK, rows),
        buf(ny - 1, TOK, head_cols),
        buf(ny - 1, TOK, head_cols),
        buf(ny, TOK, 3 * head_cols),
        buf(3, max(nx, ny, 2), 8, extra, dtype=F32),
        buf(4, TOK, rows),
        pltpu.SemaphoreType.DMA((256,)),
        pltpu.SemaphoreType.DMA((256,)),
    ]
    block_out, input_grad, grads = pl.pallas_call(
        functools.partial(layer_kernel, sizes),
        out_shape=(
            jax.ShapeDtypeStruct((TOK, rows), BF16),
            jax.ShapeDtypeStruct((TOK, rows), BF16),
            jax.ShapeDtypeStruct((8, extra), F32),
        ),
        in_specs=[hbm] * 9 + [vmem] * 4 + [hbm],
        out_specs=(vmem,) * 3,
        scratch_shapes=scratch,
        compiler_params=pltpu.CompilerParams(
            collective_id=0, has_side_effects=True, vmem_limit_bytes=60 * 1024 * 1024
        ),
    )(
        hidden_in,
        out_grad,
        q_weight,
        k_weight,
        v_weight,
        out_weight_t,
        gate_weight,
        up_weight,
        down_weight_t,
        norm_attn.reshape(blocks, 1, rows),
        norm_ffn.reshape(blocks, 1, rows),
        par,
        lens,
        position_bias,
    )
    grads = grads[0]
    return (
        block_out,
        input_grad,
        grads[:head_cols],
        grads[head_cols : 2 * head_cols],
        grads[2 * head_cols :],
    )


def solution(mesh, sizes=(4, 4, 8, 2)):
    finer = Mesh(mesh.devices.reshape(sizes), AXES)
    dp, mp = (XA, YA), (ZA, CA)
    placed = (
        P(dp, mp),
        P(dp),
        P(),
        P(dp, mp),
        P(dp, mp),
        P(dp, mp),
        P(dp, mp),
        P(),
        P(dp, mp),
        P(dp, mp),
        P(dp, mp),
        P(mp),
        P(mp),
        P(mp),
        P(dp, None),
        P(mp, None, None),
    )
    return jax.shard_map(
        functools.partial(on_device, sizes),
        mesh=finer,
        in_specs=placed,
        out_specs=(P(dp, mp), P(dp, mp), P(mp), P(mp), P(mp)),
        check_vma=False,
    )
```

```python
import functools
import math

import jax
import jax.numpy as jnp
from jax import lax
from jax.experimental import pallas as pl
from jax.experimental.pallas import tpu as pltpu
from jax.sharding import Mesh
from jax.sharding import PartitionSpec as P

HEAD_DIM = 64
EPSILON = 1e-06
NEGATIVE = -1e30
XA, YA, ZA, CA = "dp_0", "dp_1", "mp_0", "mp_1"
AXES = (XA, YA, ZA, CA)
MESH_ID = pl.DeviceIdType.MESH
F32, BF16 = jnp.float32, jnp.bfloat16
TOK = 128
CUT = 2
PART = TOK // CUT


def far_first(n):
    return sorted(range(1, n), key=lambda d: (-min(d, n - d), d))


def nn(a, b):
    return lax.dot_general(a, b, (((1,), (0,)), ((), ())), preferred_element_type=F32)


def nt(a, b):
    return lax.dot_general(a, b, (((1,), (1,)), ((), ())), preferred_element_type=F32)


def row_sums(values):
    tokens, depth = values.shape
    if tokens < TOK:
        values = jnp.concatenate([values, jnp.zeros((TOK - tokens, depth), values.dtype)], axis=0)
    return nt(jnp.ones((8, depth), BF16), values.astype(BF16))


def as_columns(row):
    return jnp.broadcast_to(row[0:1, :], (TOK, TOK)).T


def widened(col, width):
    return jnp.concatenate([col] * (width // TOK), axis=1)


class Links:
    def __init__(self, sizes, coords, send_sems, recv_sems):
        self.sizes, self.coords = sizes, coords
        self.ss, self.rs = send_sems, recv_sems
        self.used, self.sent = 0, []

    def fresh(self):
        k = self.used
        self.used += 1
        return k

    def copy(self, src, dst, device):
        k = self.fresh()
        return pltpu.make_async_remote_copy(
            src_ref=src,
            dst_ref=dst,
            send_sem=self.ss.at[k],
            recv_sem=self.rs.at[k],
            device_id=device,
            device_id_type=MESH_ID,
        )

    def start(self, src, dst, device):
        copy = self.copy(src, dst, device)
        copy.start()
        self.sent.append(copy)
        return copy

    def peer(self, axis, d):
        return lax.rem(self.coords[axis] + d, self.sizes[axis])

    def share(self, axis, ref, dst=None):
        dst = ref if dst is None else dst
        return [
            self.start(ref, dst, {axis: self.peer(axis, d)}) for d in far_first(self.sizes[axis])
        ]

    def local(self, src, dst):
        k = self.fresh()
        copy = pltpu.make_async_copy(src, dst, self.ss.at[k])
        copy.start()
        return copy


def arrived(copies):
    for copy in copies:
        copy.wait_recv()


def layer_kernel(
    sizes,
    x_in,
    og_in,
    wq_in,
    wk_in,
    wv_in,
    wo_in,
    wg_in,
    wu_in,
    wd_in,
    bias_in,
    norm_a,
    norm_f,
    sk_in,
    sv_in,
    sf_in,
    len_in,
    out_ref,
    ig_ref,
    gk_ref,
    gv_ref,
    gf_ref,
    wqkv,
    wo,
    wgu,
    wd,
    gx,
    gog,
    gn,
    sq,
    inv,
    bias_all,
    par_all,
    len_all,
    sb_qkv,
    rb_qkv,
    kv_pre,
    qkv_low,
    probs,
    gctx,
    sb_z,
    rb_z,
    fs_r,
    gfs,
    sb_gu,
    rb_gu,
    sb_dh,
    rb_dh,
    gdgu,
    ghid,
    gdot,
    pz,
    rb_dot,
    df_r,
    gdf,
    sb_dc,
    rb_dc,
    gdqkv,
    gv,
    tout,
    send_sems,
    recv_sems,
):
    nx, ny, nz, nc = sizes
    x, y, z, c = (lax.axis_index(a) for a in AXES)
    seqs = ny // nc
    s_h, hh_h = y // nc, y % nc
    a_r, s_r = z // seqs, z % seqs
    head_cols = wq_in.shape[1]
    ff_cols = wg_in.shape[1]
    rows = wq_in.shape[0]
    width = rows * nx * ny
    links = Links(dict(zip(AXES, sizes)), dict(zip(AXES, (x, y, z, c))), send_sems, recv_sems)

    partner = (x, nc * s_r + c, seqs * a_r + s_h, hh_h)
    at_home = jnp.logical_and(s_h == s_r, hh_h == c)
    away = jnp.logical_not(at_home)

    barrier = pltpu.get_barrier_semaphore()
    greeted = 0
    for axis, n in zip(AXES, sizes):
        for d in range(1, n):
            pl.semaphore_signal(
                barrier, inc=1, device_id={axis: links.peer(axis, d)}, device_id_type=MESH_ID
            )
            greeted += 1

    @pl.when(away)
    def _():
        pl.semaphore_signal(barrier, inc=1, device_id=partner, device_id_type=MESH_ID)
        pl.semaphore_wait(barrier, greeted + 1)

    @pl.when(at_home)
    def _():
        pl.semaphore_wait(barrier, greeted)

    def swapped(src, dst):
        away_copy = links.copy(src, dst, partner)
        k = links.fresh()
        home_copy = pltpu.make_async_copy(src, dst, links.ss.at[k])

        @pl.when(away)
        def _():
            away_copy.start()

        @pl.when(at_home)
        def _():
            home_copy.start()

        def done():
            @pl.when(away)
            def _():
                away_copy.wait()

            @pl.when(at_home)
            def _():
                home_copy.wait()

        return done

    z_there = seqs * a_r + s_h
    own_block = nc * z + c
    cuts = range(CUT)
    x_moved = [
        swapped(x_in.at[pl.ds(h * PART, PART), :], gx.at[h, z_there]) for h in cuts
    ]

    def w_spot(buf, col, n, there, half=None):
        start, size = there * rows, rows
        if half is not None:
            size = rows // 2
            start = start + half * size
        return buf.at[c, pl.ds(pl.multiple_of(start, size), size), pl.ds(col, n)]

    matrices = {
        "q": (wq_in, wqkv, 0),
        "k": (wk_in, wqkv, head_cols),
        "v": (wv_in, wqkv, 2 * head_cols),
        "o": (wo_in, wo, 0),
        "d": (wd_in, wd, 0),
        "g": (wg_in, wgu, 0),
        "u": (wu_in, wgu, ff_cols),
    }
    over_x, second, own_w, to_core = {}, {}, {}, {}

    def send_weights(names):
        for name in names:
            src, buf, col = matrices[name]
            spot = w_spot(buf, col, src.shape[1], x)
            steps = (1, nx - 1) if nx > 2 else range(1, nx)
            over_x[name] = {d: links.start(src, spot, {XA: links.peer(XA, d)}) for d in steps}
            own_w[name] = links.local(src, spot)
            to_core[name] = [
                links.start(src, spot, {CA: links.peer(CA, d)}) for d in range(1, nc)
            ]

    def to_other_core(name, spot):
        for e in range(1, nc):
            to_core[name].append(links.start(spot, spot, {CA: links.peer(CA, e)}))

    def relay(names):
        for name in names:
            src, buf, col = matrices[name]
            second[name] = []
            for d, copy in over_x[name].items():
                copy.wait_recv()
                there = lax.rem(x + nx - d, nx)
                if nx > 2:
                    half = 0 if d == 1 else 1
                    part = w_spot(buf, col, src.shape[1], there, half)
                    second[name].append(
                        (half, links.start(part, part, {XA: links.peer(XA, d)}))
                    )
                to_other_core(name, w_spot(buf, col, src.shape[1], there))

    def relay_far(names):
        for name in names:
            src, buf, col = matrices[name]
            for half, copy in second[name]:
                copy.wait_recv()
                to_other_core(name, w_spot(buf, col, src.shape[1], lax.rem(x + 2, nx), half))

    def weights_ready(names):
        for name in names:
            own_w[name].wait()
            arrived(to_core[name])

    send_weights("qkv")
    len_all[y] = jnp.full((8, TOK), len_in[0], jnp.int32).astype(F32)
    og_moved = [
        swapped(
            og_in.at[
                pl.ds(h * PART, PART), pl.ds(pl.multiple_of(own_block * rows, rows), rows)
            ],
            gog.at[h, z_there],
        )
        for h in cuts
    ]
    bias_here = links.local(bias_in, bias_all.at[c])
    small = links.share(CA, bias_in, bias_all.at[c])
    at = 0
    for part in (sk_in, sv_in, sf_in):
        n = part.shape[1]
        small += links.share(CA, part, par_all.at[c, :, pl.ds(at, n)])
        par_all[c, :, at : at + n] = part[...]
        at += n
    small += links.share(YA, len_all.at[y])

    x_gathered = []
    for h in cuts:
        x_moved[h]()
        x_gathered.append(links.share(ZA, gx.at[h, z]))

    def stacked(blocks, a):
        return jnp.concatenate([blocks[seqs * a + s] for s in range(seqs)], axis=0)

    def wide(blocks):
        return jnp.concatenate([stacked(blocks, a) for a in range(nx)], axis=1)

    def gain(norm, a):
        return norm[ny * a + y]

    tall = seqs * PART

    def normed(k, h, blocks, norm):
        total = None
        for a in range(nx):
            v = stacked(blocks, a).astype(F32)
            gn[h, :, a * rows : (a + 1) * rows] = (v * gain(norm, a)).astype(BF16)
            part = row_sums(v * v)
            total = part if total is None else total + part
        sq[k, h, y] = total
        return links.share(YA, sq.at[k, h, y])

    def find_inverse(k, h):
        total = sq[k, h, 0]
        for there in range(1, ny):
            total = total + sq[k, h, there]
        inv[k, h] = as_columns(lax.rsqrt(total / width + EPSILON))

    def inverse(k, h, s, n):
        spot = pl.ds(pl.multiple_of(s * PART, PART), PART)
        return widened(inv[k, h, spot, :], n)

    def scatter_y(h, lhs, weights, sent, landed):
        copies = []
        for e in range(nc - 1, -1, -1):
            hh = (hh_h + e) % nc
            part = nn(lhs, weights[hh]).astype(BF16)
            for s in range(seqs):
                sent[h, e, s] = part[s * PART : (s + 1) * PART]
            for p in range(seqs - 1, -1, -1):
                slot = e * seqs + p
                if slot:
                    s = (s_h + p) % seqs
                    copies.append(
                        links.start(
                            sent.at[h, e, s], landed.at[h, slot - 1], {YA: nc * s + hh}
                        )
                    )
        return copies

    def total_y(h, sent, landed):
        total = sent[h, 0, s_h].astype(F32)
        for slot in range(ny - 1):
            total = total + landed[h, slot].astype(F32)
        return total

    def scatter_z(k, h, held, weights, extra=None):
        copies = []
        for e in sorted(range(nx), key=lambda e: (-min(e, nx - e), e)):
            a = (a_r + e) % nx
            spot = pl.ds(pl.multiple_of(a * rows, rows), rows)
            part = None
            for hh in range(nc):
                lhs = jnp.concatenate([held[h, nc * s + hh] for s in range(seqs)], axis=0)
                term = nt(lhs, weights[hh, spot, :])
                part = term if part is None else part + term
            part = part.astype(BF16)
            for s in range(seqs):
                sb_z[k, h, e, s] = part[s * PART : (s + 1) * PART]
            for p in range(seqs):
                slot = e * seqs + p
                if slot == 0:
                    continue
                s = (s_r + p) % seqs
                there = {ZA: seqs * a + s}
                copies.append(
                    links.start(sb_z.at[k, h, e, s], rb_z.at[k, h, slot - 1], there)
                )
                if extra is not None:
                    copies.append(
                        links.start(pz.at[extra, h, s], rb_dot.at[extra, h, slot - 1], there)
                    )
        return copies

    def total_z(k, h):
        total = sb_z[k, h, 0, s_r].astype(F32)
        for slot in range(nz - 1):
            total = total + rb_z[k, h, slot].astype(F32)
        return total

    def chip_sums(k, h):
        for s in range(seqs):
            total = gdot[k, h, nc * s]
            for hh in range(1, nc):
                total = total + gdot[k, h, nc * s + hh]
            pz[k, h, s] = total

    def mean_dot(k, h):
        total = pz[k, h, s_r]
        for slot in range(nz - 1):
            total = total + rb_dot[k, h, slot]
        return widened(as_columns(total / width)[:PART], rows)

    arrived(x_gathered[0])
    sq1 = [normed(0, 0, gx.at[0], norm_a)]
    relay("qkv")
    send_weights("odgu")
    for h in range(1, CUT):
        arrived(x_gathered[h])
        sq1.append(normed(0, h, gx.at[h], norm_a))
    relay_far("qkv")
    weights_ready("qkv")
    moved = [scatter_y(h, gn[h], wqkv, sb_qkv, rb_qkv) for h in cuts]
    og_gathered = []
    for h in cuts:
        og_moved[h]()
        og_gathered.append(links.share(ZA, gog.at[h, z]))
    bias_here.wait()
    arrived(small)
    relay("o")
    par = par_all[hh_h]
    scale_key = par[:, 0:head_cols]
    scale_value = par[:, head_cols : 2 * head_cols]
    scale_ffn = par[:, 2 * head_cols : 2 * head_cols + ff_cols]
    for h in cuts:
        arrived(sq1[h])
        find_inverse(0, h)
        arrived(moved[h])
        part = pl.ds(h * PART, PART)
        raw = total_y(h, sb_qkv, rb_qkv) * inverse(0, h, s_h, 3 * head_cols)
        key_pre = raw[:, head_cols : 2 * head_cols]
        value_pre = raw[:, 2 * head_cols :]
        kv_pre[0, part, :] = key_pre
        kv_pre[1, part, :] = value_pre
        qkv_low[0, part, :] = raw[:, :head_cols].astype(BF16)
        qkv_low[1, part, :] = (key_pre * scale_key).astype(BF16)
        qkv_low[2, part, :] = (value_pre * scale_value).astype(BF16)
    lane = lax.broadcasted_iota(jnp.int32, (TOK, TOK), 1)
    real = lane.astype(F32) < len_all[nc * s_h + c][0:1, :]
    halves = [lane < HEAD_DIM, lane >= HEAD_DIM]
    zero = jnp.zeros((TOK, TOK), F32)

    def half_of(pair, half):
        return jnp.where(halves[half], pair.astype(F32), zero).astype(BF16)

    pairs = head_cols // TOK
    for pair in range(pairs):
        cols = slice(pair * TOK, (pair + 1) * TOK)
        q2, k2, v2 = (qkv_low[i, :, cols] for i in range(3))
        parts = []
        for half in range(2):
            head = 2 * pair + half
            scores = nt(half_of(q2, half), k2) + bias_all[hh_h, head]
            scores = jnp.where(real, scores, NEGATIVE)
            exponent = jnp.exp(scores - jnp.max(scores, axis=1, keepdims=True))
            prob = exponent / jnp.sum(exponent, axis=1, keepdims=True)
            probs[head] = prob
            parts.append(nn(prob.astype(BF16), v2))
        context = jnp.where(halves[0], parts[0], parts[1]).astype(BF16)
        for h in cuts:
            gctx[h, y, :, cols] = context[h * PART : (h + 1) * PART]
    ctx_gathered = [links.share(YA, gctx.at[h, y]) for h in cuts]
    relay_far("o")
    relay("d")
    weights_ready("o")
    moved = []
    for h in cuts:
        arrived(ctx_gathered[h])
        moved.append(scatter_z(0, h, gctx, wo))
    fs_gathered = []
    for h in cuts:
        arrived(moved[h])
        first_sum = gx[h, z].astype(F32) + total_z(0, h)
        fs_r[h] = first_sum
        gfs[h, z] = first_sum.astype(BF16)
        fs_gathered.append(links.share(ZA, gfs.at[h, z]))
    relay("gu")
    relay_far("d")
    weights_ready("d")
    dh_moved = []
    for h in cuts:
        arrived(og_gathered[h])
        dh_moved.append(scatter_y(h, wide(gog.at[h]), wd, sb_dh, rb_dh))
    relay_far("gu")

    sq2, moved = [], []
    for h in cuts:
        arrived(fs_gathered[h])
        sq2.append(normed(1, h, gfs.at[h], norm_f))
        if h == 0:
            weights_ready("gu")
        moved.append(scatter_y(h, gn[h], wgu, sb_gu, rb_gu))
    root = math.sqrt(2.0 / math.pi)
    dgu_gathered, dot_gathered, hid_gathered = [], [], []
    for h in cuts:
        arrived(sq2[h])
        find_inverse(1, h)
        arrived(dh_moved[h])
        d_hidden = total_y(h, sb_dh, rb_dh)
        arrived(moved[h])
        both = total_y(h, sb_gu, rb_gu) * inverse(1, h, s_h, 2 * ff_cols)
        gate, up = both[:, :ff_cols], both[:, ff_cols:]
        squared = gate * gate
        tanh = jnp.tanh(root * (gate + 0.044715 * gate * squared))
        activated = 0.5 * gate * (1.0 + tanh)
        slope = 0.5 * (1.0 + tanh) + 0.5 * gate * (1.0 - tanh * tanh) * (
            root * (1.0 + (3.0 * 0.044715) * squared)
        )
        product = activated * up
        d_product = d_hidden * scale_ffn
        d_gate = (d_product * up * slope).astype(BF16)
        d_up = (d_product * activated).astype(BF16)
        gdgu[h, y, :, :ff_cols] = d_gate
        gdgu[h, y, :, ff_cols:] = d_up
        dgu_gathered.append(links.share(YA, gdgu.at[h, y]))
        gdot[0, h, y] = row_sums(d_gate.astype(F32) * gate + d_up.astype(F32) * up)
        dot_gathered.append(links.share(YA, gdot.at[0, h, y]))
        ghid[h, y] = (product * scale_ffn).astype(BF16)
        part = jnp.sum(d_hidden * product, axis=0, keepdims=True)
        sums = part if h == 0 else sums + part
    hid_gathered = [links.share(YA, ghid.at[h, y]) for h in cuts]
    gv[0, 0, :, 2 * head_cols :] = sums
    moved = []
    for h in cuts:
        arrived(dot_gathered[h])
        chip_sums(0, h)
        arrived(dgu_gathered[h])
        moved.append(scatter_z(1, h, gdgu, wgu, 0))
    df_gathered = []
    for h in cuts:
        inv_second = inverse(1, h, s_r, rows)
        arrived(moved[h])
        d_first = (
            gog[h, z].astype(F32)
            + inv_second * (total_z(1, h) * gain(norm_f, a_r))
            - fs_r[h] * (inv_second * inv_second * mean_dot(0, h))
        )
        df_r[h] = d_first
        gdf[h, z] = d_first.astype(BF16)
        df_gathered.append(links.share(ZA, gdf.at[h, z]))

    moved = []
    for h in cuts:
        arrived(df_gathered[h])
        moved.append(scatter_y(h, wide(gdf.at[h]), wo, sb_dc, rb_dc))
    ff_moved = []
    for h in cuts:
        arrived(hid_gathered[h])
        ff_moved.append(scatter_z(2, h, ghid, wd))
    d_context = []
    for h in cuts:
        arrived(moved[h])
        d_context.append(total_y(h, sb_dc, rb_dc).astype(BF16))
    d_context = jnp.concatenate(d_context, axis=0)
    for pair in range(pairs):
        cols = slice(pair * TOK, (pair + 1) * TOK)
        q2, k2, v2 = (qkv_low[i, :, cols] for i in range(3))
        dc2 = d_context[:, cols]
        dq, dk, dv = [], [], []
        for half in range(2):
            prob = probs[2 * pair + half]
            d_probs = nt(half_of(dc2, half), v2)
            inner = jnp.sum(prob * d_probs, axis=1, keepdims=True)
            d_scores = prob * (d_probs - inner)
            dq.append(nn(d_scores.astype(BF16), k2))
            dk.append(nn(d_scores.T.astype(BF16), q2))
            dv.append(nn(prob.T.astype(BF16), dc2))
        d_query, d_key, d_value = (jnp.where(halves[0], *two) for two in (dq, dk, dv))
        key2, value2 = kv_pre[0, :, cols], kv_pre[1, :, cols]
        at = pair * TOK
        gv[0, 0, :, at : at + TOK] = jnp.sum(d_key * key2, axis=0, keepdims=True)
        at += head_cols
        gv[0, 0, :, at : at + TOK] = jnp.sum(d_value * value2, axis=0, keepdims=True)
        d_query = d_query.astype(BF16)
        d_key = (d_key * scale_key[:, cols]).astype(BF16)
        d_value = (d_value * scale_value[:, cols]).astype(BF16)
        terms = (
            d_query.astype(F32) * q2.astype(F32)
            + d_key.astype(F32) * key2
            + d_value.astype(F32) * value2
        )
        sums = [row_sums(terms[h * PART : (h + 1) * PART]) for h in cuts]
        dots = sums if pair == 0 else [old + new for old, new in zip(dots, sums)]
        for i, part in enumerate((d_query, d_key, d_value)):
            at = i * head_cols + pair * TOK
            for h in cuts:
                gdqkv[h, y, :, at : at + TOK] = part[h * PART : (h + 1) * PART]
    dqkv_gathered, dot_gathered = [], []
    for h in cuts:
        gdot[1, h, y] = dots[h]
        dot_gathered.append(links.share(YA, gdot.at[1, h, y]))
        dqkv_gathered.append(links.share(YA, gdqkv.at[h, y]))

    gv_c = links.share(CA, gv.at[0, 0], gv.at[0, 1])
    out_moved = []
    for h in cuts:
        arrived(ff_moved[h])
        tout[0, h] = (fs_r[h] + total_z(2, h)).astype(BF16)
        out_moved.append(swapped(tout.at[0, h], tout.at[2, h]))
    arrived(gv_c)
    total = gv[0, 0]
    if nc > 1:
        total = total + gv[0, 1]
    gv[1, y] = total
    gv_y = links.share(YA, gv.at[1, y])
    moved = []
    for h in cuts:
        arrived(dot_gathered[h])
        chip_sums(1, h)
        arrived(dqkv_gathered[h])
        moved.append(scatter_z(3, h, gdqkv, wqkv, 1))
    arrived(gv_y)
    total = gv[1, c]
    for s in range(1, seqs):
        total = total + gv[1, nc * s + c]
    gv[2, x] = total
    gv_x = links.share(XA, gv.at[2, x])
    ig_moved = []
    for h in cuts:
        inv_first = inverse(0, h, s_r, rows)
        arrived(moved[h])
        tout[1, h] = (
            df_r[h]
            + inv_first * (total_z(3, h) * gain(norm_a, a_r))
            - gx[h, z].astype(F32) * (inv_first * inv_first * mean_dot(1, h))
        ).astype(BF16)
        ig_moved.append(swapped(tout.at[1, h], tout.at[3, h]))
    arrived(gv_x)
    total = gv[2, 0]
    for there in range(1, nx):
        total = total + gv[2, there]
    gk_ref[...] = total[:, :head_cols]
    gv_ref[...] = total[:, head_cols : 2 * head_cols]
    gf_ref[...] = total[:, 2 * head_cols :]
    for h in cuts:
        part = pl.ds(h * PART, PART)
        out_moved[h]()
        out_ref[part, :] = tout[2, h]
        ig_moved[h]()
        ig_ref[part, :] = tout[3, h]
    for copy in links.sent:
        copy.wait_send()


def on_device(
    sizes,
    hidden_in,
    lengths,
    norm_attn,
    q_weight,
    k_weight,
    v_weight,
    out_weight_t,
    norm_ffn,
    gate_weight,
    up_weight,
    down_weight_t,
    scale_key,
    scale_value,
    scale_ffn,
    out_grad,
    position_bias,
):
    nx, ny, nz, nc = sizes
    seqs = ny // nc
    rows, head_cols = q_weight.shape
    ff_cols = gate_weight.shape[1]
    blocks = nx * ny
    extra = 2 * head_cols + ff_cols
    heads = head_cols // HEAD_DIM
    wide = rows * nx
    vmem, hbm = pl.BlockSpec(memory_space=pltpu.VMEM), pl.BlockSpec(memory_space=pl.ANY)
    smem = pl.BlockSpec(memory_space=pltpu.SMEM)

    def buf(*shape, dtype=BF16):
        return pltpu.VMEM(shape, dtype)

    scratch = [
        buf(nc, wide, 3 * head_cols),
        buf(nc, wide, head_cols),
        buf(nc, wide, 2 * ff_cols),
        buf(nc, wide, ff_cols),
        buf(CUT, nz, PART, rows),
        buf(CUT, nz, PART, rows),
        buf(CUT, seqs * PART, wide),
        buf(2, CUT, ny, 8, TOK, dtype=F32),
        buf(2, CUT, TOK, TOK, dtype=F32),
        buf(nc, heads, TOK, TOK, dtype=F32),
        buf(nc, 1, extra, dtype=F32),
        buf(ny, 8, TOK, dtype=F32),
        buf(CUT, nc, seqs, PART, 3 * head_cols),
        buf(CUT, ny - 1, PART, 3 * head_cols),
        buf(2, TOK, head_cols, dtype=F32),
        buf(3, TOK, head_cols),
        buf(heads, TOK, TOK, dtype=F32),
        buf(CUT, ny, PART, head_cols),
        buf(4, CUT, nx, seqs, PART, rows),
        buf(4, CUT, nz - 1, PART, rows),
        buf(CUT, PART, rows, dtype=F32),
        buf(CUT, nz, PART, rows),
        buf(CUT, nc, seqs, PART, 2 * ff_cols),
        buf(CUT, ny - 1, PART, 2 * ff_cols),
        buf(CUT, nc, seqs, PART, ff_cols),
        buf(CUT, ny - 1, PART, ff_cols),
        buf(CUT, ny, PART, 2 * ff_cols),
        buf(CUT, ny, PART, ff_cols),
        buf(2, CUT, ny, 8, TOK, dtype=F32),
        buf(2, CUT, seqs, 8, TOK, dtype=F32),
        buf(2, CUT, nz - 1, 8, TOK, dtype=F32),
        buf(CUT, PART, rows, dtype=F32),
        buf(CUT, nz, PART, rows),
        buf(CUT, nc, seqs, PART, head_cols),
        buf(CUT, ny - 1, PART, head_cols),
        buf(CUT, ny, PART, 3 * head_cols),
        buf(3, max(nx, ny, 2), 1, extra, dtype=F32),
        buf(4, CUT, PART, rows),
        pltpu.SemaphoreType.DMA((448,)),
        pltpu.SemaphoreType.DMA((448,)),
    ]
    block_out, input_grad, grad_key, grad_value, grad_ffn = pl.pallas_call(
        functools.partial(layer_kernel, sizes),
        out_shape=(
            jax.ShapeDtypeStruct((TOK, rows), BF16),
            jax.ShapeDtypeStruct((TOK, rows), BF16),
            jax.ShapeDtypeStruct((1, head_cols), F32),
            jax.ShapeDtypeStruct((1, head_cols), F32),
            jax.ShapeDtypeStruct((1, ff_cols), F32),
        ),
        in_specs=[hbm] * 10 + [vmem] * 5 + [smem],
        out_specs=(vmem,) * 5,
        scratch_shapes=scratch,
        compiler_params=pltpu.CompilerParams(
            collective_id=0, has_side_effects=True, vmem_limit_bytes=60 * 1024 * 1024
        ),
    )(
        hidden_in,
        out_grad,
        q_weight,
        k_weight,
        v_weight,
        out_weight_t,
        gate_weight,
        up_weight,
        down_weight_t,
        position_bias,
        norm_attn.reshape(blocks, 1, rows),
        norm_ffn.reshape(blocks, 1, rows),
        scale_key[None],
        scale_value[None],
        scale_ffn[None],
        lengths,
    )
    return block_out, input_grad, grad_key[0], grad_value[0], grad_ffn[0]


def solution(mesh, sizes=(4, 4, 8, 2)):
    finer = Mesh(mesh.devices.reshape(sizes), AXES)
    dp, mp = (XA, YA), (ZA, CA)
    placed = (
        P(dp, mp),
        P(dp),
        P(),
        P(dp, mp),
        P(dp, mp),
        P(dp, mp),
        P(dp, mp),
        P(),
        P(dp, mp),
        P(dp, mp),
        P(dp, mp),
        P(mp),
        P(mp),
        P(mp),
        P(dp, None),
        P(mp, None, None),
    )
    return jax.shard_map(
        functools.partial(on_device, sizes),
        mesh=finer,
        in_specs=placed,
        out_specs=(P(dp, mp), P(dp, mp), P(mp), P(mp), P(mp)),
        check_vma=False,
    )
```

```python
import functools
import math

import jax
import jax.numpy as jnp
from jax import lax
from jax.experimental import pallas as pl
from jax.experimental.pallas import tpu as pltpu
from jax.sharding import Mesh
from jax.sharding import PartitionSpec as P

HEAD_DIM = 64
EPSILON = 1e-06
NEGATIVE = -1e30
XA, YA, ZA, CA = "dp_0", "dp_1", "mp_0", "mp_1"
AXES = (XA, YA, ZA, CA)
MESH_ID = pl.DeviceIdType.MESH
F32, BF16 = jnp.float32, jnp.bfloat16
TOK = 128
CUT = 4
PART = TOK // CUT


def far_first(n):
    return sorted(range(1, n), key=lambda d: (-min(d, n - d), d))


def nn(a, b):
    return lax.dot_general(a, b, (((1,), (0,)), ((), ())), preferred_element_type=F32)


def nt(a, b):
    return lax.dot_general(a, b, (((1,), (1,)), ((), ())), preferred_element_type=F32)


def row_sums(values):
    tokens, depth = values.shape
    if tokens < TOK:
        values = jnp.concatenate([values, jnp.zeros((TOK - tokens, depth), values.dtype)], axis=0)
    return nt(jnp.ones((8, depth), BF16), values.astype(BF16))


def as_columns(row):
    return jnp.broadcast_to(row[0:1, :], (TOK, TOK)).T


def widened(col, width):
    return jnp.concatenate([col] * (width // TOK), axis=1)


class Links:
    def __init__(self, sizes, coords, send_sems, recv_sems):
        self.sizes, self.coords = sizes, coords
        self.ss, self.rs = send_sems, recv_sems
        self.used, self.sent = 0, []

    def fresh(self):
        k = self.used
        self.used += 1
        return k

    def copy(self, src, dst, device):
        k = self.fresh()
        return pltpu.make_async_remote_copy(
            src_ref=src,
            dst_ref=dst,
            send_sem=self.ss.at[k],
            recv_sem=self.rs.at[k],
            device_id=device,
            device_id_type=MESH_ID,
        )

    def start(self, src, dst, device):
        copy = self.copy(src, dst, device)
        copy.start()
        self.sent.append(copy)
        return copy

    def peer(self, axis, d):
        return lax.rem(self.coords[axis] + d, self.sizes[axis])

    def share(self, axis, ref, dst=None):
        dst = ref if dst is None else dst
        return [
            self.start(ref, dst, {axis: self.peer(axis, d)}) for d in far_first(self.sizes[axis])
        ]

    def local(self, src, dst):
        k = self.fresh()
        copy = pltpu.make_async_copy(src, dst, self.ss.at[k])
        copy.start()
        return copy


def arrived(copies):
    for copy in copies:
        copy.wait_recv()


def layer_kernel(
    sizes,
    x_in,
    og_in,
    wq_in,
    wk_in,
    wv_in,
    wo_in,
    wg_in,
    wu_in,
    wd_in,
    bias_in,
    norm_a,
    norm_f,
    sk_in,
    sv_in,
    sf_in,
    len_in,
    out_ref,
    ig_ref,
    gk_ref,
    gv_ref,
    gf_ref,
    wqkv,
    wo,
    wgu,
    wd,
    gx,
    gog,
    gn,
    sq,
    inv,
    bias_all,
    par_all,
    len_all,
    sb_qkv,
    rb_qkv,
    kv_pre,
    qkv_low,
    probs,
    gctx,
    sb_z,
    rb_z,
    fs_r,
    gfs,
    sb_gu,
    rb_gu,
    sb_dh,
    rb_dh,
    gdgu,
    ghid,
    gdot,
    pz,
    rb_dot,
    df_r,
    gdf,
    sb_dc,
    rb_dc,
    gdqkv,
    gv,
    tout,
    send_sems,
    recv_sems,
):
    nx, ny, nz, nc = sizes
    x, y, z, c = (lax.axis_index(a) for a in AXES)
    seqs = ny // nc
    s_h, hh_h = y // nc, y % nc
    a_r, s_r = z // seqs, z % seqs
    head_cols = wq_in.shape[1]
    ff_cols = wg_in.shape[1]
    rows = wq_in.shape[0]
    width = rows * nx * ny
    links = Links(dict(zip(AXES, sizes)), dict(zip(AXES, (x, y, z, c))), send_sems, recv_sems)

    partner = (x, nc * s_r + c, seqs * a_r + s_h, hh_h)
    at_home = jnp.logical_and(s_h == s_r, hh_h == c)
    away = jnp.logical_not(at_home)

    barrier = pltpu.get_barrier_semaphore()
    greeted = 0
    for axis, n in zip(AXES, sizes):
        for d in range(1, n):
            pl.semaphore_signal(
                barrier, inc=1, device_id={axis: links.peer(axis, d)}, device_id_type=MESH_ID
            )
            greeted += 1

    @pl.when(away)
    def _():
        pl.semaphore_signal(barrier, inc=1, device_id=partner, device_id_type=MESH_ID)
        pl.semaphore_wait(barrier, greeted + 1)

    @pl.when(at_home)
    def _():
        pl.semaphore_wait(barrier, greeted)

    def swapped(src, dst):
        away_copy = links.copy(src, dst, partner)
        k = links.fresh()
        home_copy = pltpu.make_async_copy(src, dst, links.ss.at[k])

        @pl.when(away)
        def _():
            away_copy.start()

        @pl.when(at_home)
        def _():
            home_copy.start()

        def done():
            @pl.when(away)
            def _():
                away_copy.wait()

            @pl.when(at_home)
            def _():
                home_copy.wait()

        return done

    z_there = seqs * a_r + s_h
    own_block = nc * z + c
    cuts = range(CUT)
    x_moved = [
        swapped(x_in.at[pl.ds(h * PART, PART), :], gx.at[h, z_there]) for h in cuts
    ]

    def w_spot(buf, col, n, there, half=None):
        start, size = there * rows, rows
        if half is not None:
            size = rows // 2
            start = start + half * size
        return buf.at[c, pl.ds(pl.multiple_of(start, size), size), pl.ds(col, n)]

    matrices = {
        "q": (wq_in, wqkv, 0),
        "k": (wk_in, wqkv, head_cols),
        "v": (wv_in, wqkv, 2 * head_cols),
        "o": (wo_in, wo, 0),
        "d": (wd_in, wd, 0),
        "g": (wg_in, wgu, 0),
        "u": (wu_in, wgu, ff_cols),
    }
    over_x, second, own_w, to_core = {}, {}, {}, {}

    def send_weights(names):
        for name in names:
            src, buf, col = matrices[name]
            spot = w_spot(buf, col, src.shape[1], x)
            steps = (1, nx - 1) if nx > 2 else range(1, nx)
            over_x[name] = {d: links.start(src, spot, {XA: links.peer(XA, d)}) for d in steps}
            own_w[name] = links.local(src, spot)
            to_core[name] = [
                links.start(src, spot, {CA: links.peer(CA, d)}) for d in range(1, nc)
            ]

    def to_other_core(name, spot):
        for e in range(1, nc):
            to_core[name].append(links.start(spot, spot, {CA: links.peer(CA, e)}))

    def relay(names):
        for name in names:
            src, buf, col = matrices[name]
            second[name] = []
            for d, copy in over_x[name].items():
                copy.wait_recv()
                there = lax.rem(x + nx - d, nx)
                if nx > 2:
                    half = 0 if d == 1 else 1
                    part = w_spot(buf, col, src.shape[1], there, half)
                    second[name].append(
                        (half, links.start(part, part, {XA: links.peer(XA, d)}))
                    )
                to_other_core(name, w_spot(buf, col, src.shape[1], there))

    def relay_far(names):
        for name in names:
            src, buf, col = matrices[name]
            for half, copy in second[name]:
                copy.wait_recv()
                to_other_core(name, w_spot(buf, col, src.shape[1], lax.rem(x + 2, nx), half))

    def weights_ready(names):
        for name in names:
            own_w[name].wait()
            arrived(to_core[name])

    send_weights("qkvo")
    len_all[y] = jnp.full((8, TOK), len_in[0], jnp.int32).astype(F32)
    og_moved = [
        swapped(
            og_in.at[
                pl.ds(h * PART, PART), pl.ds(pl.multiple_of(own_block * rows, rows), rows)
            ],
            gog.at[h, z_there],
        )
        for h in cuts
    ]
    bias_here = links.local(bias_in, bias_all.at[c])
    small = links.share(CA, bias_in, bias_all.at[c])
    at = 0
    for part in (sk_in, sv_in, sf_in):
        n = part.shape[1]
        small += links.share(CA, part, par_all.at[c, :, pl.ds(at, n)])
        par_all[c, :, at : at + n] = part[...]
        at += n
    small += links.share(YA, len_all.at[y])

    x_gathered = []
    for h in cuts:
        x_moved[h]()
        x_gathered.append(links.share(ZA, gx.at[h, z]))
    relay("qkvo")
    send_weights("dgu")

    def stacked(blocks, a):
        return jnp.concatenate([blocks[seqs * a + s] for s in range(seqs)], axis=0)

    def wide(blocks):
        return jnp.concatenate([stacked(blocks, a) for a in range(nx)], axis=1)

    def gain(norm, a):
        return norm[ny * a + y]

    tall = seqs * PART

    def normed(k, h, blocks, norm):
        total = None
        for a in range(nx):
            v = stacked(blocks, a).astype(F32)
            gn[h, :, a * rows : (a + 1) * rows] = (v * gain(norm, a)).astype(BF16)
            part = row_sums(v * v)
            total = part if total is None else total + part
        sq[k, h, y] = total
        return links.share(YA, sq.at[k, h, y])

    def find_inverse(k, h):
        total = sq[k, h, 0]
        for there in range(1, ny):
            total = total + sq[k, h, there]
        inv[k, h] = as_columns(lax.rsqrt(total / width + EPSILON))

    def inverse(k, h, s, n):
        spot = pl.ds(pl.multiple_of(s * PART, PART), PART)
        return widened(inv[k, h, spot, :], n)

    def scatter_y(h, lhs, weights, sent, landed):
        copies = []
        for e in range(nc - 1, -1, -1):
            hh = (hh_h + e) % nc
            part = nn(lhs, weights[hh]).astype(BF16)
            for s in range(seqs):
                sent[h, e, s] = part[s * PART : (s + 1) * PART]
            for p in range(seqs - 1, -1, -1):
                slot = e * seqs + p
                if slot:
                    s = (s_h + p) % seqs
                    copies.append(
                        links.start(
                            sent.at[h, e, s], landed.at[h, slot - 1], {YA: nc * s + hh}
                        )
                    )
        return copies

    def total_y(h, sent, landed):
        total = sent[h, 0, s_h].astype(F32)
        for slot in range(ny - 1):
            total = total + landed[h, slot].astype(F32)
        return total

    def scatter_z(k, h, held, weights, extra=None):
        copies = []
        for e in sorted(range(nx), key=lambda e: (-min(e, nx - e), e)):
            a = (a_r + e) % nx
            spot = pl.ds(pl.multiple_of(a * rows, rows), rows)
            part = None
            for hh in range(nc):
                lhs = jnp.concatenate([held[h, nc * s + hh] for s in range(seqs)], axis=0)
                term = nt(lhs, weights[hh, spot, :])
                part = term if part is None else part + term
            part = part.astype(BF16)
            for s in range(seqs):
                sb_z[k, h, e, s] = part[s * PART : (s + 1) * PART]
            for p in range(seqs):
                slot = e * seqs + p
                if slot == 0:
                    continue
                s = (s_r + p) % seqs
                there = {ZA: seqs * a + s}
                copies.append(
                    links.start(sb_z.at[k, h, e, s], rb_z.at[k, h, slot - 1], there)
                )
                if extra is not None:
                    copies.append(
                        links.start(pz.at[extra, h, s], rb_dot.at[extra, h, slot - 1], there)
                    )
        return copies

    def total_z(k, h):
        total = sb_z[k, h, 0, s_r].astype(F32)
        for slot in range(nz - 1):
            total = total + rb_z[k, h, slot].astype(F32)
        return total

    def chip_sums(k, h):
        for s in range(seqs):
            total = gdot[k, h, nc * s]
            for hh in range(1, nc):
                total = total + gdot[k, h, nc * s + hh]
            pz[k, h, s] = total

    def mean_dot(k, h):
        total = pz[k, h, s_r]
        for slot in range(nz - 1):
            total = total + rb_dot[k, h, slot]
        return widened(as_columns(total / width)[:PART], rows)

    arrived(x_gathered[0])
    sq1 = [normed(0, 0, gx.at[0], norm_a)]
    for h in range(1, CUT):
        arrived(x_gathered[h])
        sq1.append(normed(0, h, gx.at[h], norm_a))
    relay_far("qkv")
    weights_ready("qkv")
    moved = [scatter_y(h, gn[h], wqkv, sb_qkv, rb_qkv) for h in cuts]
    og_gathered = []
    for h in cuts:
        og_moved[h]()
        og_gathered.append(links.share(ZA, gog.at[h, z]))
    bias_here.wait()
    arrived(small)
    relay_far("o")
    weights_ready("o")
    relay("d")
    par = par_all[hh_h]
    scale_key = par[:, 0:head_cols]
    scale_value = par[:, head_cols : 2 * head_cols]
    scale_ffn = par[:, 2 * head_cols : 2 * head_cols + ff_cols]
    for h in cuts:
        arrived(sq1[h])
        find_inverse(0, h)
        arrived(moved[h])
        part = pl.ds(h * PART, PART)
        raw = total_y(h, sb_qkv, rb_qkv) * inverse(0, h, s_h, 3 * head_cols)
        key_pre = raw[:, head_cols : 2 * head_cols]
        value_pre = raw[:, 2 * head_cols :]
        kv_pre[0, part, :] = key_pre
        kv_pre[1, part, :] = value_pre
        qkv_low[0, part, :] = raw[:, :head_cols].astype(BF16)
        qkv_low[1, part, :] = (key_pre * scale_key).astype(BF16)
        qkv_low[2, part, :] = (value_pre * scale_value).astype(BF16)
    lane = lax.broadcasted_iota(jnp.int32, (TOK, TOK), 1)
    real = lane.astype(F32) < len_all[nc * s_h + c][0:1, :]
    halves = [lane < HEAD_DIM, lane >= HEAD_DIM]
    zero = jnp.zeros((TOK, TOK), F32)

    def half_of(pair, half):
        return jnp.where(halves[half], pair.astype(F32), zero).astype(BF16)

    pairs = head_cols // TOK
    for pair in range(pairs):
        cols = slice(pair * TOK, (pair + 1) * TOK)
        q2, k2, v2 = (qkv_low[i, :, cols] for i in range(3))
        parts = []
        for half in range(2):
            head = 2 * pair + half
            scores = nt(half_of(q2, half), k2) + bias_all[hh_h, head]
            scores = jnp.where(real, scores, NEGATIVE)
            exponent = jnp.exp(scores - jnp.max(scores, axis=1, keepdims=True))
            prob = exponent / jnp.sum(exponent, axis=1, keepdims=True)
            probs[head] = prob
            parts.append(nn(prob.astype(BF16), v2))
        context = jnp.where(halves[0], parts[0], parts[1]).astype(BF16)
        for h in cuts:
            gctx[h, y, :, cols] = context[h * PART : (h + 1) * PART]
    ctx_gathered = [links.share(YA, gctx.at[h, y]) for h in cuts]

    root = math.sqrt(2.0 / math.pi)
    out_sums, first, second_norm, hidden_dots = {}, {}, {}, {}
    partial, dgu_gathered, hid_gathered, d_out, df_gathered, dc_moved = {}, {}, {}, {}, {}, {}
    dh_moved, sums = {}, []

    def out_product(h):
        arrived(ctx_gathered[h])
        out_sums[h] = scatter_z(0, h, gctx, wo)

    def first_residual(h):
        arrived(out_sums[h])
        first_sum = gx[h, z].astype(F32) + total_z(0, h)
        fs_r[h] = first_sum
        gfs[h, z] = first_sum.astype(BF16)
        first[h] = links.share(ZA, gfs.at[h, z])

    def hidden_grads():
        relay("gu")
        relay_far("d")
        weights_ready("d")
        for h in cuts:
            arrived(og_gathered[h])
            dh_moved[h] = scatter_y(h, wide(gog.at[h]), wd, sb_dh, rb_dh)
        relay_far("gu")

    def gate_and_up(h):
        if h == 0:
            hidden_grads()
        arrived(first[h])
        second_norm[h] = normed(1, h, gfs.at[h], norm_f)
        if h == 0:
            weights_ready("gu")
        partial[h] = scatter_y(h, gn[h], wgu, sb_gu, rb_gu)

    def hidden_units(h):
        arrived(second_norm[h])
        find_inverse(1, h)
        arrived(dh_moved[h])
        d_hidden = total_y(h, sb_dh, rb_dh)
        arrived(partial[h])
        both = total_y(h, sb_gu, rb_gu) * inverse(1, h, s_h, 2 * ff_cols)
        gate, up = both[:, :ff_cols], both[:, ff_cols:]
        squared = gate * gate
        tanh = jnp.tanh(root * (gate + 0.044715 * gate * squared))
        activated = 0.5 * gate * (1.0 + tanh)
        slope = 0.5 * (1.0 + tanh) + 0.5 * gate * (1.0 - tanh * tanh) * (
            root * (1.0 + (3.0 * 0.044715) * squared)
        )
        product = activated * up
        d_product = d_hidden * scale_ffn
        d_gate = (d_product * up * slope).astype(BF16)
        d_up = (d_product * activated).astype(BF16)
        gdgu[h, y, :, :ff_cols] = d_gate
        gdgu[h, y, :, ff_cols:] = d_up
        dgu_gathered[h] = links.share(YA, gdgu.at[h, y])
        gdot[0, h, y] = row_sums(d_gate.astype(F32) * gate + d_up.astype(F32) * up)
        hidden_dots[h] = links.share(YA, gdot.at[0, h, y])
        ghid[h, y] = (product * scale_ffn).astype(BF16)
        sums.append(jnp.sum(d_hidden * product, axis=0, keepdims=True))
        if h == CUT - 1:
            for i in cuts:
                hid_gathered[i] = links.share(YA, ghid.at[i, y])
            total = sums[0]
            for part in sums[1:]:
                total = total + part
            gv[0, 0, :, 2 * head_cols :] = total

    def second_grad(h):
        arrived(hidden_dots[h])
        chip_sums(0, h)
        arrived(dgu_gathered[h])
        d_out[h] = scatter_z(1, h, gdgu, wgu, 0)

    def first_grad(h):
        inv_second = inverse(1, h, s_r, rows)
        arrived(d_out[h])
        d_first = (
            gog[h, z].astype(F32)
            + inv_second * (total_z(1, h) * gain(norm_f, a_r))
            - fs_r[h] * (inv_second * inv_second * mean_dot(0, h))
        )
        df_r[h] = d_first
        gdf[h, z] = d_first.astype(BF16)
        df_gathered[h] = links.share(ZA, gdf.at[h, z])

    def context_grad(h):
        arrived(df_gathered[h])
        dc_moved[h] = scatter_y(h, wide(gdf.at[h]), wo, sb_dc, rb_dc)

    wave = (
        out_product,
        first_residual,
        gate_and_up,
        hidden_units,
        second_grad,
        first_grad,
        context_grad,
    )
    for step in range(len(wave) + CUT - 1):
        for k, stage in enumerate(wave):
            if 0 <= step - k < CUT:
                stage(step - k)
    ff_moved = []
    for h in cuts:
        arrived(hid_gathered[h])
        ff_moved.append(scatter_z(2, h, ghid, wd))
    d_context = []
    for h in cuts:
        arrived(dc_moved[h])
        d_context.append(total_y(h, sb_dc, rb_dc).astype(BF16))
    d_context = jnp.concatenate(d_context, axis=0)
    for pair in range(pairs):
        cols = slice(pair * TOK, (pair + 1) * TOK)
        q2, k2, v2 = (qkv_low[i, :, cols] for i in range(3))
        dc2 = d_context[:, cols]
        dq, dk, dv = [], [], []
        for half in range(2):
            prob = probs[2 * pair + half]
            d_probs = nt(half_of(dc2, half), v2)
            inner = jnp.sum(prob * d_probs, axis=1, keepdims=True)
            d_scores = prob * (d_probs - inner)
            dq.append(nn(d_scores.astype(BF16), k2))
            dk.append(nn(d_scores.T.astype(BF16), q2))
            dv.append(nn(prob.T.astype(BF16), dc2))
        d_query, d_key, d_value = (jnp.where(halves[0], *two) for two in (dq, dk, dv))
        key2, value2 = kv_pre[0, :, cols], kv_pre[1, :, cols]
        at = pair * TOK
        gv[0, 0, :, at : at + TOK] = jnp.sum(d_key * key2, axis=0, keepdims=True)
        at += head_cols
        gv[0, 0, :, at : at + TOK] = jnp.sum(d_value * value2, axis=0, keepdims=True)
        d_query = d_query.astype(BF16)
        d_key = (d_key * scale_key[:, cols]).astype(BF16)
        d_value = (d_value * scale_value[:, cols]).astype(BF16)
        terms = (
            d_query.astype(F32) * q2.astype(F32)
            + d_key.astype(F32) * key2
            + d_value.astype(F32) * value2
        )
        sums = [row_sums(terms[h * PART : (h + 1) * PART]) for h in cuts]
        dots = sums if pair == 0 else [old + new for old, new in zip(dots, sums)]
        for i, part in enumerate((d_query, d_key, d_value)):
            at = i * head_cols + pair * TOK
            for h in cuts:
                gdqkv[h, y, :, at : at + TOK] = part[h * PART : (h + 1) * PART]
    dqkv_gathered, dot_gathered = [], []
    for h in cuts:
        gdot[1, h, y] = dots[h]
        dot_gathered.append(links.share(YA, gdot.at[1, h, y]))
        dqkv_gathered.append(links.share(YA, gdqkv.at[h, y]))

    gv_c = links.share(CA, gv.at[0, 0], gv.at[0, 1])
    out_moved = []
    for h in cuts:
        arrived(ff_moved[h])
        tout[0, h] = (fs_r[h] + total_z(2, h)).astype(BF16)
        out_moved.append(swapped(tout.at[0, h], tout.at[2, h]))
    arrived(gv_c)
    total = gv[0, 0]
    if nc > 1:
        total = total + gv[0, 1]
    gv[1, y] = total
    gv_y = links.share(YA, gv.at[1, y])
    moved = []
    for h in cuts:
        arrived(dot_gathered[h])
        chip_sums(1, h)
        arrived(dqkv_gathered[h])
        moved.append(scatter_z(3, h, gdqkv, wqkv, 1))
    arrived(gv_y)
    total = gv[1, c]
    for s in range(1, seqs):
        total = total + gv[1, nc * s + c]
    gv[2, x] = total
    gv_x = links.share(XA, gv.at[2, x])
    ig_moved = []
    for h in cuts:
        inv_first = inverse(0, h, s_r, rows)
        arrived(moved[h])
        tout[1, h] = (
            df_r[h]
            + inv_first * (total_z(3, h) * gain(norm_a, a_r))
            - gx[h, z].astype(F32) * (inv_first * inv_first * mean_dot(1, h))
        ).astype(BF16)
        ig_moved.append(swapped(tout.at[1, h], tout.at[3, h]))
    arrived(gv_x)
    total = gv[2, 0]
    for there in range(1, nx):
        total = total + gv[2, there]
    gk_ref[...] = total[:, :head_cols]
    gv_ref[...] = total[:, head_cols : 2 * head_cols]
    gf_ref[...] = total[:, 2 * head_cols :]
    for h in cuts:
        part = pl.ds(h * PART, PART)
        out_moved[h]()
        out_ref[part, :] = tout[2, h]
        ig_moved[h]()
        ig_ref[part, :] = tout[3, h]
    for copy in links.sent:
        copy.wait_send()


def publish_kernel(out_in, ig_in, gk_in, gv_in, gf_in, out_ref, ig_ref, gk_ref, gv_ref, gf_ref):
    out_ref[...] = out_in[...]
    ig_ref[...] = ig_in[...]
    gk_ref[...] = gk_in[...]
    gv_ref[...] = gv_in[...]
    gf_ref[...] = gf_in[0]


def on_device(
    sizes,
    hidden_in,
    lengths,
    norm_attn,
    q_weight,
    k_weight,
    v_weight,
    out_weight_t,
    norm_ffn,
    gate_weight,
    up_weight,
    down_weight_t,
    scale_key,
    scale_value,
    scale_ffn,
    out_grad,
    position_bias,
):
    nx, ny, nz, nc = sizes
    seqs = ny // nc
    rows, head_cols = q_weight.shape
    ff_cols = gate_weight.shape[1]
    blocks = nx * ny
    extra = 2 * head_cols + ff_cols
    heads = head_cols // HEAD_DIM
    wide = rows * nx
    vmem, hbm = pl.BlockSpec(memory_space=pltpu.VMEM), pl.BlockSpec(memory_space=pl.ANY)
    smem = pl.BlockSpec(memory_space=pltpu.SMEM)

    def buf(*shape, dtype=BF16):
        return pltpu.VMEM(shape, dtype)

    scratch = [
        buf(nc, wide, 3 * head_cols),
        buf(nc, wide, head_cols),
        buf(nc, wide, 2 * ff_cols),
        buf(nc, wide, ff_cols),
        buf(CUT, nz, PART, rows),
        buf(CUT, nz, PART, rows),
        buf(CUT, seqs * PART, wide),
        buf(2, CUT, ny, 8, TOK, dtype=F32),
        buf(2, CUT, TOK, TOK, dtype=F32),
        buf(nc, heads, TOK, TOK, dtype=F32),
        buf(nc, 1, extra, dtype=F32),
        buf(ny, 8, TOK, dtype=F32),
        buf(CUT, nc, seqs, PART, 3 * head_cols),
        buf(CUT, ny - 1, PART, 3 * head_cols),
        buf(2, TOK, head_cols, dtype=F32),
        buf(3, TOK, head_cols),
        buf(heads, TOK, TOK, dtype=F32),
        buf(CUT, ny, PART, head_cols),
        buf(4, CUT, nx, seqs, PART, rows),
        buf(4, CUT, nz - 1, PART, rows),
        buf(CUT, PART, rows, dtype=F32),
        buf(CUT, nz, PART, rows),
        buf(CUT, nc, seqs, PART, 2 * ff_cols),
        buf(CUT, ny - 1, PART, 2 * ff_cols),
        buf(CUT, nc, seqs, PART, ff_cols),
        buf(CUT, ny - 1, PART, ff_cols),
        buf(CUT, ny, PART, 2 * ff_cols),
        buf(CUT, ny, PART, ff_cols),
        buf(2, CUT, ny, 8, TOK, dtype=F32),
        buf(2, CUT, seqs, 8, TOK, dtype=F32),
        buf(2, CUT, nz - 1, 8, TOK, dtype=F32),
        buf(CUT, PART, rows, dtype=F32),
        buf(CUT, nz, PART, rows),
        buf(CUT, nc, seqs, PART, head_cols),
        buf(CUT, ny - 1, PART, head_cols),
        buf(CUT, ny, PART, 3 * head_cols),
        buf(3, max(nx, ny, 2), 1, extra, dtype=F32),
        buf(4, CUT, PART, rows),
        pltpu.SemaphoreType.DMA((640,)),
        pltpu.SemaphoreType.DMA((640,)),
    ]
    block_out, input_grad, grad_key, grad_value, grad_ffn = pl.pallas_call(
        functools.partial(layer_kernel, sizes),
        out_shape=(
            jax.ShapeDtypeStruct((TOK, rows), BF16),
            jax.ShapeDtypeStruct((TOK, rows), BF16),
            jax.ShapeDtypeStruct((1, head_cols), F32),
            jax.ShapeDtypeStruct((1, head_cols), F32),
            jax.ShapeDtypeStruct((1, ff_cols), F32),
        ),
        in_specs=[hbm] * 10 + [vmem] * 5 + [smem],
        out_specs=(vmem,) * 5,
        scratch_shapes=scratch,
        compiler_params=pltpu.CompilerParams(
            collective_id=0, has_side_effects=True, vmem_limit_bytes=60 * 1024 * 1024
        ),
    )(
        hidden_in,
        out_grad,
        q_weight,
        k_weight,
        v_weight,
        out_weight_t,
        gate_weight,
        up_weight,
        down_weight_t,
        position_bias,
        norm_attn.reshape(blocks, 1, rows),
        norm_ffn.reshape(blocks, 1, rows),
        scale_key[None],
        scale_value[None],
        scale_ffn[None],
        lengths,
    )
    results = pl.pallas_call(
        publish_kernel,
        out_shape=(
            jax.ShapeDtypeStruct((TOK, rows), BF16),
            jax.ShapeDtypeStruct((TOK, rows), BF16),
            jax.ShapeDtypeStruct((1, head_cols), F32),
            jax.ShapeDtypeStruct((1, head_cols), F32),
            jax.ShapeDtypeStruct((ff_cols,), F32),
        ),
        in_specs=[vmem] * 5,
        out_specs=(vmem,) * 5,
    )(block_out, input_grad, grad_key, grad_value, grad_ffn)
    block_out, input_grad, grad_key, grad_value, grad_ffn = results
    return block_out, input_grad, grad_key[0], grad_value[0], grad_ffn


def solution(mesh, sizes=(4, 4, 8, 2)):
    finer = Mesh(mesh.devices.reshape(sizes), AXES)
    dp, mp = (XA, YA), (ZA, CA)
    placed = (
        P(dp, mp),
        P(dp),
        P(),
        P(dp, mp),
        P(dp, mp),
        P(dp, mp),
        P(dp, mp),
        P(),
        P(dp, mp),
        P(dp, mp),
        P(dp, mp),
        P(mp),
        P(mp),
        P(mp),
        P(dp, None),
        P(mp, None, None),
    )
    return jax.shard_map(
        functools.partial(on_device, sizes),
        mesh=finer,
        in_specs=placed,
        out_specs=(P(dp, mp), P(dp, mp), P(mp), P(mp), P(mp)),
        check_vma=False,
    )
```

```python
import functools
import math

import jax
import jax.numpy as jnp
from jax import lax
from jax.experimental import pallas as pl
from jax.experimental.pallas import tpu as pltpu
from jax.sharding import Mesh
from jax.sharding import PartitionSpec as P

HEAD_DIM = 64
EPSILON = 1e-06
NEGATIVE = -1e30
XA, YA, ZA, CA = "dp_0", "dp_1", "mp_0", "mp_1"
AXES = (XA, YA, ZA, CA)
MESH_ID = pl.DeviceIdType.MESH
F32, BF16 = jnp.float32, jnp.bfloat16
TOK = 128
CUT = 4
PART = TOK // CUT


def far_first(n):
    return sorted(range(1, n), key=lambda d: (min(d, n - d), d))


def nn(a, b):
    return lax.dot_general(a, b, (((1,), (0,)), ((), ())), preferred_element_type=F32)


def nt(a, b):
    return lax.dot_general(a, b, (((1,), (1,)), ((), ())), preferred_element_type=F32)


def row_sums(values):
    tokens, depth = values.shape
    if tokens < TOK:
        values = jnp.concatenate([values, jnp.zeros((TOK - tokens, depth), values.dtype)], axis=0)
    return nt(jnp.ones((8, depth), BF16), values.astype(BF16))[0:1]


def as_columns(row):
    return jnp.broadcast_to(row, (TOK, TOK)).T


def widened(col, width):
    return jnp.concatenate([col] * (width // TOK), axis=1)


class Links:
    def __init__(self, sizes, coords, send_sems, recv_sems):
        self.sizes, self.coords = sizes, coords
        self.ss, self.rs = send_sems, recv_sems
        self.used, self.sent = 0, []

    def fresh(self):
        k = self.used
        self.used += 1
        return k

    def copy(self, src, dst, device):
        k = self.fresh()
        return pltpu.make_async_remote_copy(
            src_ref=src,
            dst_ref=dst,
            send_sem=self.ss.at[k],
            recv_sem=self.rs.at[k],
            device_id=device,
            device_id_type=MESH_ID,
        )

    def start(self, src, dst, device):
        copy = self.copy(src, dst, device)
        copy.start()
        self.sent.append(copy)
        return copy

    def peer(self, axis, d):
        return lax.rem(self.coords[axis] + d, self.sizes[axis])

    def share(self, axis, ref, dst=None):
        dst = ref if dst is None else dst
        return [
            self.start(ref, dst, {axis: self.peer(axis, d)}) for d in far_first(self.sizes[axis])
        ]

    def local(self, src, dst):
        k = self.fresh()
        copy = pltpu.make_async_copy(src, dst, self.ss.at[k])
        copy.start()
        return copy


def arrived(copies):
    for copy in copies:
        copy.wait_recv()


def layer_kernel(
    sizes,
    x_in,
    og_in,
    wq_in,
    wk_in,
    wv_in,
    wo_in,
    wg_in,
    wu_in,
    wd_in,
    bias_in,
    norm_a,
    norm_f,
    sk_in,
    sv_in,
    sf_in,
    len_in,
    out_ref,
    ig_ref,
    gk_ref,
    gv_ref,
    gf_ref,
    wqkv,
    wo,
    wgu,
    wd,
    gx,
    gog,
    gn,
    sq,
    inv,
    bias_all,
    par_all,
    len_all,
    sb_qkv,
    rb_qkv,
    kv_pre,
    qkv_low,
    probs,
    gctx,
    sb_z,
    rb_z,
    fs_r,
    gfs,
    sb_gu,
    rb_gu,
    sb_dh,
    rb_dh,
    gdgu,
    ghid,
    gdot,
    pz,
    rb_dot,
    df_r,
    gdf,
    sb_dc,
    rb_dc,
    gdqkv,
    gv,
    tout,
    send_sems,
    recv_sems,
):
    nx, ny, nz, nc = sizes
    x, y, z, c = (lax.axis_index(a) for a in AXES)
    seqs = ny // nc
    s_h, hh_h = y // nc, y % nc
    a_r, s_r = z // seqs, z % seqs
    head_cols = wq_in.shape[1]
    ff_cols = wg_in.shape[1]
    rows = wq_in.shape[0]
    width = rows * nx * ny
    links = Links(dict(zip(AXES, sizes)), dict(zip(AXES, (x, y, z, c))), send_sems, recv_sems)

    partner = (x, nc * s_r + c, seqs * a_r + s_h, hh_h)
    at_home = jnp.logical_and(s_h == s_r, hh_h == c)
    away = jnp.logical_not(at_home)

    barrier = pltpu.get_barrier_semaphore()
    greeted = 0
    for axis, n in zip(AXES, sizes):
        for d in range(1, n):
            pl.semaphore_signal(
                barrier, inc=1, device_id={axis: links.peer(axis, d)}, device_id_type=MESH_ID
            )
            greeted += 1

    @pl.when(away)
    def _():
        pl.semaphore_signal(barrier, inc=1, device_id=partner, device_id_type=MESH_ID)
        pl.semaphore_wait(barrier, greeted + 1)

    @pl.when(at_home)
    def _():
        pl.semaphore_wait(barrier, greeted)

    def swapped(src, dst):
        away_copy = links.copy(src, dst, partner)
        k = links.fresh()
        home_copy = pltpu.make_async_copy(src, dst, links.ss.at[k])

        @pl.when(away)
        def _():
            away_copy.start()

        @pl.when(at_home)
        def _():
            home_copy.start()

        def done():
            @pl.when(away)
            def _():
                away_copy.wait()

            @pl.when(at_home)
            def _():
                home_copy.wait()

        return done

    z_there = seqs * a_r + s_h
    own_block = nc * z + c
    cuts = range(CUT)
    x_moved = [
        swapped(x_in.at[pl.ds(h * PART, PART), :], gx.at[h, z_there]) for h in cuts
    ]

    def w_spot(buf, col, n, there, half=None):
        start, size = there * rows, rows
        if half is not None:
            size = rows // 2
            start = start + half * size
        return buf.at[c, pl.ds(pl.multiple_of(start, size), size), pl.ds(col, n)]

    matrices = {
        "q": (wq_in, wqkv, 0),
        "k": (wk_in, wqkv, head_cols),
        "v": (wv_in, wqkv, 2 * head_cols),
        "o": (wo_in, wo, 0),
        "d": (wd_in, wd, 0),
        "g": (wg_in, wgu, 0),
        "u": (wu_in, wgu, ff_cols),
    }
    over_x, second, own_w, to_core = {}, {}, {}, {}

    def send_weights(names):
        for name in names:
            src, buf, col = matrices[name]
            spot = w_spot(buf, col, src.shape[1], x)
            steps = (1, nx - 1) if nx > 2 else range(1, nx)
            over_x[name] = {d: links.start(src, spot, {XA: links.peer(XA, d)}) for d in steps}
            own_w[name] = links.local(src, spot)
            to_core[name] = [
                links.start(src, spot, {CA: links.peer(CA, d)}) for d in range(1, nc)
            ]

    def to_other_core(name, spot):
        for e in range(1, nc):
            to_core[name].append(links.start(spot, spot, {CA: links.peer(CA, e)}))

    def relay(names):
        for name in names:
            src, buf, col = matrices[name]
            second[name] = []
            for d, copy in over_x[name].items():
                copy.wait_recv()
                there = lax.rem(x + nx - d, nx)
                if nx > 2:
                    half = 0 if d == 1 else 1
                    part = w_spot(buf, col, src.shape[1], there, half)
                    second[name].append(
                        (half, links.start(part, part, {XA: links.peer(XA, d)}))
                    )
                to_other_core(name, w_spot(buf, col, src.shape[1], there))

    def relay_far(names):
        for name in names:
            src, buf, col = matrices[name]
            for half, copy in second[name]:
                copy.wait_recv()
                to_other_core(name, w_spot(buf, col, src.shape[1], lax.rem(x + 2, nx), half))

    def weights_ready(names):
        for name in names:
            own_w[name].wait()
            arrived(to_core[name])

    send_weights("qkvo")
    len_all[y] = jnp.full((1, TOK), len_in[0], jnp.int32).astype(F32)
    og_moved = [
        swapped(
            og_in.at[
                pl.ds(h * PART, PART), pl.ds(pl.multiple_of(own_block * rows, rows), rows)
            ],
            gog.at[h, z_there],
        )
        for h in cuts
    ]
    bias_here = links.local(bias_in, bias_all.at[c])
    small = links.share(CA, bias_in, bias_all.at[c])
    at = 0
    for part in (sk_in, sv_in, sf_in):
        n = part.shape[1]
        small += links.share(CA, part, par_all.at[c, :, pl.ds(at, n)])
        par_all[c, :, at : at + n] = part[...]
        at += n
    small += links.share(YA, len_all.at[y])

    x_gathered = []
    for h in cuts:
        x_moved[h]()
        x_gathered.append(links.share(ZA, gx.at[h, z]))
    relay("qkvo")
    send_weights("dgu")

    def stacked(blocks, a):
        return jnp.concatenate([blocks[seqs * a + s] for s in range(seqs)], axis=0)

    def wide(blocks):
        return jnp.concatenate([stacked(blocks, a) for a in range(nx)], axis=1)

    def gain(norm, a):
        return norm[ny * a + y]

    tall = seqs * PART

    def normed(k, h, blocks, norm):
        total = None
        for a in range(nx):
            v = stacked(blocks, a).astype(F32)
            gn[h, :, a * rows : (a + 1) * rows] = (v * gain(norm, a)).astype(BF16)
            part = row_sums(v * v)
            total = part if total is None else total + part
        sq[k, h, y] = total
        return links.share(YA, sq.at[k, h, y])

    def find_inverse(k, h):
        total = sq[k, h, 0]
        for there in range(1, ny):
            total = total + sq[k, h, there]
        inv[k, h] = as_columns(lax.rsqrt(total / width + EPSILON))

    def inverse(k, h, s, n):
        spot = pl.ds(pl.multiple_of(s * PART, PART), PART)
        return widened(inv[k, h, spot, :], n)

    def scatter_y(h, lhs, weights, sent, landed):
        copies = []
        for e in range(nc - 1, -1, -1):
            hh = (hh_h + e) % nc
            part = nn(lhs, weights[hh]).astype(BF16)
            for s in range(seqs):
                sent[h, e, s] = part[s * PART : (s + 1) * PART]
            for p in range(seqs - 1, -1, -1):
                slot = e * seqs + p
                if slot:
                    s = (s_h + p) % seqs
                    copies.append(
                        links.start(
                            sent.at[h, e, s], landed.at[h, slot - 1], {YA: nc * s + hh}
                        )
                    )
        return copies

    def total_y(h, sent, landed):
        total = sent[h, 0, s_h].astype(F32)
        for slot in range(ny - 1):
            total = total + landed[h, slot].astype(F32)
        return total

    def scatter_z(k, h, held, weights, extra=None):
        copies = []
        for e in sorted(range(nx), key=lambda e: (-min(e, nx - e), e)):
            a = (a_r + e) % nx
            spot = pl.ds(pl.multiple_of(a * rows, rows), rows)
            part = None
            for hh in range(nc):
                lhs = jnp.concatenate([held[h, nc * s + hh] for s in range(seqs)], axis=0)
                term = nt(lhs, weights[hh, spot, :])
                part = term if part is None else part + term
            part = part.astype(BF16)
            for s in range(seqs):
                sb_z[k, h, e, s] = part[s * PART : (s + 1) * PART]
            for p in range(seqs):
                slot = e * seqs + p
                if slot == 0:
                    continue
                s = (s_r + p) % seqs
                there = {ZA: seqs * a + s}
                copies.append(
                    links.start(sb_z.at[k, h, e, s], rb_z.at[k, h, slot - 1], there)
                )
                if extra is not None:
                    copies.append(
                        links.start(pz.at[extra, h, s], rb_dot.at[extra, h, slot - 1], there)
                    )
        return copies

    def total_z(k, h):
        total = sb_z[k, h, 0, s_r].astype(F32)
        for slot in range(nz - 1):
            total = total + rb_z[k, h, slot].astype(F32)
        return total

    def chip_sums(k, h):
        for s in range(seqs):
            total = gdot[k, h, nc * s]
            for hh in range(1, nc):
                total = total + gdot[k, h, nc * s + hh]
            pz[k, h, s] = total

    def mean_dot(k, h):
        total = pz[k, h, s_r]
        for slot in range(nz - 1):
            total = total + rb_dot[k, h, slot]
        return widened(as_columns(total / width)[:PART], rows)

    arrived(x_gathered[0])
    sq1 = [normed(0, 0, gx.at[0], norm_a)]
    for h in range(1, CUT):
        arrived(x_gathered[h])
        sq1.append(normed(0, h, gx.at[h], norm_a))
    relay_far("qkv")
    weights_ready("qkv")
    moved = [scatter_y(h, gn[h], wqkv, sb_qkv, rb_qkv) for h in cuts]
    og_gathered = []
    for h in cuts:
        og_moved[h]()
        og_gathered.append(links.share(ZA, gog.at[h, z]))
    bias_here.wait()
    arrived(small)
    relay_far("o")
    weights_ready("o")
    relay("d")
    par = par_all[hh_h]
    scale_key = par[:, 0:head_cols]
    scale_value = par[:, head_cols : 2 * head_cols]
    scale_ffn = par[:, 2 * head_cols : 2 * head_cols + ff_cols]
    for h in cuts:
        arrived(sq1[h])
        find_inverse(0, h)
        arrived(moved[h])
        part = pl.ds(h * PART, PART)
        raw = total_y(h, sb_qkv, rb_qkv) * inverse(0, h, s_h, 3 * head_cols)
        key_pre = raw[:, head_cols : 2 * head_cols]
        value_pre = raw[:, 2 * head_cols :]
        kv_pre[0, part, :] = key_pre
        kv_pre[1, part, :] = value_pre
        qkv_low[0, part, :] = raw[:, :head_cols].astype(BF16)
        qkv_low[1, part, :] = (key_pre * scale_key).astype(BF16)
        qkv_low[2, part, :] = (value_pre * scale_value).astype(BF16)
    lane = lax.broadcasted_iota(jnp.int32, (TOK, TOK), 1)
    real = lane.astype(F32) < len_all[nc * s_h + c]
    halves = [lane < HEAD_DIM, lane >= HEAD_DIM]
    zero = jnp.zeros((TOK, TOK), F32)

    def half_of(pair, half):
        return jnp.where(halves[half], pair.astype(F32), zero).astype(BF16)

    pairs = head_cols // TOK
    for pair in range(pairs):
        cols = slice(pair * TOK, (pair + 1) * TOK)
        q2, k2, v2 = (qkv_low[i, :, cols] for i in range(3))
        parts = []
        for half in range(2):
            head = 2 * pair + half
            scores = nt(half_of(q2, half), k2) + bias_all[hh_h, head]
            scores = jnp.where(real, scores, NEGATIVE)
            exponent = jnp.exp(scores - jnp.max(scores, axis=1, keepdims=True))
            prob = exponent / jnp.sum(exponent, axis=1, keepdims=True)
            probs[head] = prob
            parts.append(nn(prob.astype(BF16), v2))
        context = jnp.where(halves[0], parts[0], parts[1]).astype(BF16)
        for h in cuts:
            gctx[h, y, :, cols] = context[h * PART : (h + 1) * PART]
    ctx_gathered = [links.share(YA, gctx.at[h, y]) for h in cuts]

    root = math.sqrt(2.0 / math.pi)
    out_sums, first, second_norm, hidden_dots = {}, {}, {}, {}
    partial, dgu_gathered, hid_gathered, d_out, df_gathered, dc_moved = {}, {}, {}, {}, {}, {}
    dh_moved, sums = {}, []

    def out_product(h):
        arrived(ctx_gathered[h])
        out_sums[h] = scatter_z(0, h, gctx, wo)

    def first_residual(h):
        arrived(out_sums[h])
        first_sum = gx[h, z].astype(F32) + total_z(0, h)
        fs_r[h] = first_sum
        gfs[h, z] = first_sum.astype(BF16)
        first[h] = links.share(ZA, gfs.at[h, z])

    def hidden_grads():
        relay("gu")
        relay_far("d")
        weights_ready("d")
        for h in cuts:
            arrived(og_gathered[h])
            dh_moved[h] = scatter_y(h, wide(gog.at[h]), wd, sb_dh, rb_dh)
        relay_far("gu")

    def gate_and_up(h):
        if h == 0:
            hidden_grads()
        arrived(first[h])
        second_norm[h] = normed(1, h, gfs.at[h], norm_f)
        if h == 0:
            weights_ready("gu")
        partial[h] = scatter_y(h, gn[h], wgu, sb_gu, rb_gu)

    def hidden_units(h):
        arrived(second_norm[h])
        find_inverse(1, h)
        arrived(dh_moved[h])
        d_hidden = total_y(h, sb_dh, rb_dh)
        arrived(partial[h])
        both = total_y(h, sb_gu, rb_gu) * inverse(1, h, s_h, 2 * ff_cols)
        gate, up = both[:, :ff_cols], both[:, ff_cols:]
        squared = gate * gate
        tanh = jnp.tanh(root * (gate + 0.044715 * gate * squared))
        activated = 0.5 * gate * (1.0 + tanh)
        slope = 0.5 * (1.0 + tanh) + 0.5 * gate * (1.0 - tanh * tanh) * (
            root * (1.0 + (3.0 * 0.044715) * squared)
        )
        product = activated * up
        d_product = d_hidden * scale_ffn
        d_gate = (d_product * up * slope).astype(BF16)
        d_up = (d_product * activated).astype(BF16)
        gdgu[h, y, :, :ff_cols] = d_gate
        gdgu[h, y, :, ff_cols:] = d_up
        dgu_gathered[h] = links.share(YA, gdgu.at[h, y])
        gdot[0, h, y] = row_sums(d_gate.astype(F32) * gate + d_up.astype(F32) * up)
        hidden_dots[h] = links.share(YA, gdot.at[0, h, y])
        ghid[h, y] = (product * scale_ffn).astype(BF16)
        sums.append(jnp.sum(d_hidden * product, axis=0, keepdims=True))
        if h == CUT - 1:
            for i in cuts:
                hid_gathered[i] = links.share(YA, ghid.at[i, y])
            total = sums[0]
            for part in sums[1:]:
                total = total + part
            gv[0, 0, :, 2 * head_cols :] = total

    def second_grad(h):
        arrived(hidden_dots[h])
        chip_sums(0, h)
        arrived(dgu_gathered[h])
        d_out[h] = scatter_z(1, h, gdgu, wgu, 0)

    def first_grad(h):
        inv_second = inverse(1, h, s_r, rows)
        arrived(d_out[h])
        d_first = (
            gog[h, z].astype(F32)
            + inv_second * (total_z(1, h) * gain(norm_f, a_r))
            - fs_r[h] * (inv_second * inv_second * mean_dot(0, h))
        )
        df_r[h] = d_first
        gdf[h, z] = d_first.astype(BF16)
        df_gathered[h] = links.share(ZA, gdf.at[h, z])

    def context_grad(h):
        arrived(df_gathered[h])
        dc_moved[h] = scatter_y(h, wide(gdf.at[h]), wo, sb_dc, rb_dc)

    wave = (
        out_product,
        first_residual,
        gate_and_up,
        hidden_units,
        second_grad,
        first_grad,
        context_grad,
    )
    for step in range(len(wave) + CUT - 1):
        for k, stage in enumerate(wave):
            if 0 <= step - k < CUT:
                stage(step - k)
    ff_moved = []
    for h in cuts:
        arrived(hid_gathered[h])
        ff_moved.append(scatter_z(2, h, ghid, wd))
    d_context = []
    for h in cuts:
        arrived(dc_moved[h])
        d_context.append(total_y(h, sb_dc, rb_dc).astype(BF16))
    d_context = jnp.concatenate(d_context, axis=0)
    for pair in range(pairs):
        cols = slice(pair * TOK, (pair + 1) * TOK)
        q2, k2, v2 = (qkv_low[i, :, cols] for i in range(3))
        dc2 = d_context[:, cols]
        dq, dk, dv = [], [], []
        for half in range(2):
            prob = probs[2 * pair + half]
            d_probs = nt(half_of(dc2, half), v2)
            inner = jnp.sum(prob * d_probs, axis=1, keepdims=True)
            d_scores = prob * (d_probs - inner)
            dq.append(nn(d_scores.astype(BF16), k2))
            dk.append(nn(d_scores.T.astype(BF16), q2))
            dv.append(nn(prob.T.astype(BF16), dc2))
        d_query, d_key, d_value = (jnp.where(halves[0], *two) for two in (dq, dk, dv))
        key2, value2 = kv_pre[0, :, cols], kv_pre[1, :, cols]
        at = pair * TOK
        gv[0, 0, :, at : at + TOK] = jnp.sum(d_key * key2, axis=0, keepdims=True)
        at += head_cols
        gv[0, 0, :, at : at + TOK] = jnp.sum(d_value * value2, axis=0, keepdims=True)
        d_query = d_query.astype(BF16)
        d_key = (d_key * scale_key[:, cols]).astype(BF16)
        d_value = (d_value * scale_value[:, cols]).astype(BF16)
        terms = (
            d_query.astype(F32) * q2.astype(F32)
            + d_key.astype(F32) * key2
            + d_value.astype(F32) * value2
        )
        sums = [row_sums(terms[h * PART : (h + 1) * PART]) for h in cuts]
        dots = sums if pair == 0 else [old + new for old, new in zip(dots, sums)]
        for i, part in enumerate((d_query, d_key, d_value)):
            at = i * head_cols + pair * TOK
            for h in cuts:
                gdqkv[h, y, :, at : at + TOK] = part[h * PART : (h + 1) * PART]
    dqkv_gathered, dot_gathered = [], []
    for h in cuts:
        gdot[1, h, y] = dots[h]
        dot_gathered.append(links.share(YA, gdot.at[1, h, y]))
        dqkv_gathered.append(links.share(YA, gdqkv.at[h, y]))

    gv_c = links.share(CA, gv.at[0, 0], gv.at[0, 1])
    out_moved = []
    for h in cuts:
        arrived(ff_moved[h])
        tout[0, h] = (fs_r[h] + total_z(2, h)).astype(BF16)
        out_moved.append(swapped(tout.at[0, h], tout.at[2, h]))
    arrived(gv_c)
    total = gv[0, 0]
    if nc > 1:
        total = total + gv[0, 1]
    gv[1, y] = total
    gv_y = links.share(YA, gv.at[1, y])
    moved = []
    for h in cuts:
        arrived(dot_gathered[h])
        chip_sums(1, h)
        arrived(dqkv_gathered[h])
        moved.append(scatter_z(3, h, gdqkv, wqkv, 1))
    arrived(gv_y)
    total = gv[1, c]
    for s in range(1, seqs):
        total = total + gv[1, nc * s + c]
    gv[2, x] = total
    gv_x = links.share(XA, gv.at[2, x])
    ig_moved = []
    for h in cuts:
        inv_first = inverse(0, h, s_r, rows)
        arrived(moved[h])
        tout[1, h] = (
            df_r[h]
            + inv_first * (total_z(3, h) * gain(norm_a, a_r))
            - gx[h, z].astype(F32) * (inv_first * inv_first * mean_dot(1, h))
        ).astype(BF16)
        ig_moved.append(swapped(tout.at[1, h], tout.at[3, h]))
    arrived(gv_x)
    total = gv[2, 0]
    for there in range(1, nx):
        total = total + gv[2, there]
    gk_ref[...] = total[:, :head_cols]
    gv_ref[...] = total[:, head_cols : 2 * head_cols]
    gf_ref[...] = total[:, 2 * head_cols :]
    for h in cuts:
        part = pl.ds(h * PART, PART)
        out_moved[h]()
        out_ref[part, :] = tout[2, h]
        ig_moved[h]()
        ig_ref[part, :] = tout[3, h]
    for copy in links.sent:
        copy.wait_send()


def publish_kernel(out_in, ig_in, gk_in, gv_in, gf_in, out_ref, ig_ref, gk_ref, gv_ref, gf_ref):
    out_ref[...] = out_in[...]
    ig_ref[...] = ig_in[...]
    gk_ref[...] = gk_in[...]
    gv_ref[...] = gv_in[...]
    gf_ref[...] = gf_in[0]


def on_device(
    sizes,
    hidden_in,
    lengths,
    norm_attn,
    q_weight,
    k_weight,
    v_weight,
    out_weight_t,
    norm_ffn,
    gate_weight,
    up_weight,
    down_weight_t,
    scale_key,
    scale_value,
    scale_ffn,
    out_grad,
    position_bias,
):
    nx, ny, nz, nc = sizes
    seqs = ny // nc
    rows, head_cols = q_weight.shape
    ff_cols = gate_weight.shape[1]
    blocks = nx * ny
    extra = 2 * head_cols + ff_cols
    heads = head_cols // HEAD_DIM
    wide = rows * nx
    vmem, hbm = pl.BlockSpec(memory_space=pltpu.VMEM), pl.BlockSpec(memory_space=pl.ANY)
    smem = pl.BlockSpec(memory_space=pltpu.SMEM)

    def buf(*shape, dtype=BF16):
        return pltpu.VMEM(shape, dtype)

    scratch = [
        buf(nc, wide, 3 * head_cols),
        buf(nc, wide, head_cols),
        buf(nc, wide, 2 * ff_cols),
        buf(nc, wide, ff_cols),
        buf(CUT, nz, PART, rows),
        buf(CUT, nz, PART, rows),
        buf(CUT, seqs * PART, wide),
        buf(2, CUT, ny, 1, TOK, dtype=F32),
        buf(2, CUT, TOK, TOK, dtype=F32),
        buf(nc, heads, TOK, TOK, dtype=F32),
        buf(nc, 1, extra, dtype=F32),
        buf(ny, 1, TOK, dtype=F32),
        buf(CUT, nc, seqs, PART, 3 * head_cols),
        buf(CUT, ny - 1, PART, 3 * head_cols),
        buf(2, TOK, head_cols, dtype=F32),
        buf(3, TOK, head_cols),
        buf(heads, TOK, TOK, dtype=F32),
        buf(CUT, ny, PART, head_cols),
        buf(4, CUT, nx, seqs, PART, rows),
        buf(4, CUT, nz - 1, PART, rows),
        buf(CUT, PART, rows, dtype=F32),
        buf(CUT, nz, PART, rows),
        buf(CUT, nc, seqs, PART, 2 * ff_cols),
        buf(CUT, ny - 1, PART, 2 * ff_cols),
        buf(CUT, nc, seqs, PART, ff_cols),
        buf(CUT, ny - 1, PART, ff_cols),
        buf(CUT, ny, PART, 2 * ff_cols),
        buf(CUT, ny, PART, ff_cols),
        buf(2, CUT, ny, 1, TOK, dtype=F32),
        buf(2, CUT, seqs, 1, TOK, dtype=F32),
        buf(2, CUT, nz - 1, 1, TOK, dtype=F32),
        buf(CUT, PART, rows, dtype=F32),
        buf(CUT, nz, PART, rows),
        buf(CUT, nc, seqs, PART, head_cols),
        buf(CUT, ny - 1, PART, head_cols),
        buf(CUT, ny, PART, 3 * head_cols),
        buf(3, max(nx, ny, 2), 1, extra, dtype=F32),
        buf(4, CUT, PART, rows),
        pltpu.SemaphoreType.DMA((640,)),
        pltpu.SemaphoreType.DMA((640,)),
    ]
    block_out, input_grad, grad_key, grad_value, grad_ffn = pl.pallas_call(
        functools.partial(layer_kernel, sizes),
        out_shape=(
            jax.ShapeDtypeStruct((TOK, rows), BF16),
            jax.ShapeDtypeStruct((TOK, rows), BF16),
            jax.ShapeDtypeStruct((1, head_cols), F32),
            jax.ShapeDtypeStruct((1, head_cols), F32),
            jax.ShapeDtypeStruct((1, ff_cols), F32),
        ),
        in_specs=[hbm] * 10 + [vmem] * 5 + [smem],
        out_specs=(vmem,) * 5,
        scratch_shapes=scratch,
        compiler_params=pltpu.CompilerParams(
            collective_id=0, has_side_effects=True, vmem_limit_bytes=60 * 1024 * 1024
        ),
    )(
        hidden_in,
        out_grad,
        q_weight,
        k_weight,
        v_weight,
        out_weight_t,
        gate_weight,
        up_weight,
        down_weight_t,
        position_bias,
        norm_attn.reshape(blocks, 1, rows),
        norm_ffn.reshape(blocks, 1, rows),
        scale_key[None],
        scale_value[None],
        scale_ffn[None],
        lengths,
    )
    results = pl.pallas_call(
        publish_kernel,
        out_shape=(
            jax.ShapeDtypeStruct((TOK, rows), BF16),
            jax.ShapeDtypeStruct((TOK, rows), BF16),
            jax.ShapeDtypeStruct((1, head_cols), F32),
            jax.ShapeDtypeStruct((1, head_cols), F32),
            jax.ShapeDtypeStruct((ff_cols,), F32),
        ),
        in_specs=[vmem] * 5,
        out_specs=(vmem,) * 5,
    )(block_out, input_grad, grad_key, grad_value, grad_ffn)
    block_out, input_grad, grad_key, grad_value, grad_ffn = results
    return block_out, input_grad, grad_key[0], grad_value[0], grad_ffn


def solution(mesh, sizes=(4, 4, 8, 2)):
    finer = Mesh(mesh.devices.reshape(sizes), AXES)
    dp, mp = (XA, YA), (ZA, CA)
    placed = (
        P(dp, mp),
        P(dp),
        P(),
        P(dp, mp),
        P(dp, mp),
        P(dp, mp),
        P(dp, mp),
        P(),
        P(dp, mp),
        P(dp, mp),
        P(dp, mp),
        P(mp),
        P(mp),
        P(mp),
        P(dp, None),
        P(mp, None, None),
    )
    return jax.shard_map(
        functools.partial(on_device, sizes),
        mesh=finer,
        in_specs=placed,
        out_specs=(P(dp, mp), P(dp, mp), P(mp), P(mp), P(mp)),
        check_vma=False,
    )
```

```python
import functools
import math

import jax
import jax.numpy as jnp
from jax import lax
from jax.experimental import pallas as pl
from jax.experimental.pallas import tpu as pltpu
from jax.sharding import Mesh
from jax.sharding import PartitionSpec as P

HEAD_DIM = 64
EPSILON = 1e-06
NEGATIVE = -1e30
XA, YA, ZA, CA = "dp_0", "dp_1", "mp_0", "mp_1"
AXES = (XA, YA, ZA, CA)
MESH_ID = pl.DeviceIdType.MESH
F32, BF16 = jnp.float32, jnp.bfloat16
TOK = 128
CUT = 4
PART = TOK // CUT


def far_first(n):
    return sorted(range(1, n), key=lambda d: (min(d, n - d), d))


def nn(a, b):
    return lax.dot_general(a, b, (((1,), (0,)), ((), ())), preferred_element_type=F32)


def nt(a, b):
    return lax.dot_general(a, b, (((1,), (1,)), ((), ())), preferred_element_type=F32)


def row_sums(values):
    tokens, depth = values.shape
    if tokens < TOK:
        values = jnp.concatenate([values, jnp.zeros((TOK - tokens, depth), values.dtype)], axis=0)
    return nt(jnp.ones((8, depth), BF16), values.astype(BF16))[0:1]


def as_columns(row):
    return jnp.broadcast_to(row, (TOK, TOK)).T


def widened(col, width):
    return jnp.concatenate([col] * (width // TOK), axis=1)


class Links:
    def __init__(self, sizes, coords, send_sems, recv_sems):
        self.sizes, self.coords = sizes, coords
        self.ss, self.rs = send_sems, recv_sems
        self.used, self.sent = 0, []

    def fresh(self):
        k = self.used
        self.used += 1
        return k

    def copy(self, src, dst, device):
        k = self.fresh()
        return pltpu.make_async_remote_copy(
            src_ref=src,
            dst_ref=dst,
            send_sem=self.ss.at[k],
            recv_sem=self.rs.at[k],
            device_id=device,
            device_id_type=MESH_ID,
        )

    def start(self, src, dst, device):
        copy = self.copy(src, dst, device)
        copy.start()
        self.sent.append(copy)
        return copy

    def peer(self, axis, d):
        return lax.rem(self.coords[axis] + d, self.sizes[axis])

    def share(self, axis, ref, dst=None):
        dst = ref if dst is None else dst
        return [
            self.start(ref, dst, {axis: self.peer(axis, d)}) for d in far_first(self.sizes[axis])
        ]

    def local(self, src, dst):
        k = self.fresh()
        copy = pltpu.make_async_copy(src, dst, self.ss.at[k])
        copy.start()
        return copy


def arrived(copies):
    for copy in copies:
        copy.wait_recv()


def layer_kernel(
    sizes,
    x_in,
    og_in,
    wq_in,
    wk_in,
    wv_in,
    wo_in,
    wg_in,
    wu_in,
    wd_in,
    bias_in,
    norm_a,
    norm_f,
    sk_in,
    sv_in,
    sf_in,
    len_in,
    out_ref,
    ig_ref,
    gk_ref,
    gv_ref,
    gf_ref,
    wqkv,
    wo,
    wgu,
    wd,
    gx,
    gog,
    gn,
    sq,
    inv,
    bias_all,
    par_all,
    len_all,
    sb_qkv,
    rb_qkv,
    kv_pre,
    qkv_low,
    probs,
    gctx,
    sb_z,
    rb_z,
    fs_r,
    gfs,
    sb_gu,
    rb_gu,
    sb_dh,
    rb_dh,
    gdgu,
    ghid,
    gdot,
    pz,
    rb_dot,
    df_r,
    gdf,
    sb_dc,
    rb_dc,
    gdqkv,
    gv,
    tout,
    send_sems,
    recv_sems,
):
    nx, ny, nz, nc = sizes
    x, y, z, c = (lax.axis_index(a) for a in AXES)
    seqs = ny // nc
    s_h, hh_h = y // nc, y % nc
    a_r, s_r = z // seqs, z % seqs
    head_cols = wq_in.shape[1]
    ff_cols = wg_in.shape[1]
    rows = wq_in.shape[0]
    width = rows * nx * ny
    links = Links(dict(zip(AXES, sizes)), dict(zip(AXES, (x, y, z, c))), send_sems, recv_sems)

    partner = (x, nc * s_r + c, seqs * a_r + s_h, hh_h)
    at_home = jnp.logical_and(s_h == s_r, hh_h == c)
    away = jnp.logical_not(at_home)

    barrier = pltpu.get_barrier_semaphore()
    greeted = 0
    for axis, n in zip(AXES, sizes):
        for d in range(1, n):
            pl.semaphore_signal(
                barrier, inc=1, device_id={axis: links.peer(axis, d)}, device_id_type=MESH_ID
            )
            greeted += 1

    @pl.when(away)
    def _():
        pl.semaphore_signal(barrier, inc=1, device_id=partner, device_id_type=MESH_ID)
        pl.semaphore_wait(barrier, greeted + 1)

    @pl.when(at_home)
    def _():
        pl.semaphore_wait(barrier, greeted)

    def swapped(src, dst):
        away_copy = links.copy(src, dst, partner)
        k = links.fresh()
        home_copy = pltpu.make_async_copy(src, dst, links.ss.at[k])

        @pl.when(away)
        def _():
            away_copy.start()

        @pl.when(at_home)
        def _():
            home_copy.start()

        def done():
            @pl.when(away)
            def _():
                away_copy.wait()

            @pl.when(at_home)
            def _():
                home_copy.wait()

        return done

    z_there = seqs * a_r + s_h
    own_block = nc * z + c
    cuts = range(CUT)
    x_moved = [
        swapped(x_in.at[pl.ds(h * PART, PART), :], gx.at[h, z_there]) for h in cuts
    ]

    def w_spot(buf, col, n, there, half=None):
        start, size = there * rows, rows
        if half is not None:
            size = rows // 2
            start = start + half * size
        return buf.at[c, pl.ds(pl.multiple_of(start, size), size), pl.ds(col, n)]

    matrices = {
        "q": (wq_in, wqkv, 0),
        "k": (wk_in, wqkv, head_cols),
        "v": (wv_in, wqkv, 2 * head_cols),
        "o": (wo_in, wo, 0),
        "d": (wd_in, wd, 0),
        "g": (wg_in, wgu, 0),
        "u": (wu_in, wgu, ff_cols),
    }
    over_x, second, own_w, to_core = {}, {}, {}, {}

    def send_weights(names):
        for name in names:
            src, buf, col = matrices[name]
            spot = w_spot(buf, col, src.shape[1], x)
            steps = (1, nx - 1) if nx > 2 else range(1, nx)
            over_x[name] = {d: links.start(src, spot, {XA: links.peer(XA, d)}) for d in steps}
            own_w[name] = links.local(src, spot)
            to_core[name] = [
                links.start(src, spot, {CA: links.peer(CA, d)}) for d in range(1, nc)
            ]

    def to_other_core(name, spot):
        for e in range(1, nc):
            to_core[name].append(links.start(spot, spot, {CA: links.peer(CA, e)}))

    def relay(names):
        for name in names:
            src, buf, col = matrices[name]
            second[name] = []
            for d, copy in over_x[name].items():
                copy.wait_recv()
                there = lax.rem(x + nx - d, nx)
                if nx > 2:
                    half = 0 if d == 1 else 1
                    part = w_spot(buf, col, src.shape[1], there, half)
                    second[name].append(
                        (half, links.start(part, part, {XA: links.peer(XA, d)}))
                    )
                to_other_core(name, w_spot(buf, col, src.shape[1], there))

    def relay_far(names):
        for name in names:
            src, buf, col = matrices[name]
            for half, copy in second[name]:
                copy.wait_recv()
                to_other_core(name, w_spot(buf, col, src.shape[1], lax.rem(x + 2, nx), half))

    def weights_ready(names):
        for name in names:
            own_w[name].wait()
            arrived(to_core[name])

    send_weights("qkv")
    len_all[y] = jnp.full((1, TOK), len_in[0], jnp.int32).astype(F32)
    og_moved = [
        swapped(
            og_in.at[
                pl.ds(h * PART, PART), pl.ds(pl.multiple_of(own_block * rows, rows), rows)
            ],
            gog.at[h, z_there],
        )
        for h in cuts
    ]
    bias_here = links.local(bias_in, bias_all.at[c])
    small = links.share(CA, bias_in, bias_all.at[c])
    at = 0
    for part in (sk_in, sv_in, sf_in):
        n = part.shape[1]
        small += links.share(CA, part, par_all.at[c, :, pl.ds(at, n)])
        par_all[c, :, at : at + n] = part[...]
        at += n
    small += links.share(YA, len_all.at[y])

    x_gathered = []
    for h in cuts:
        x_moved[h]()
        x_gathered.append(links.share(ZA, gx.at[h, z]))
    relay("qkv")
    send_weights("o")

    def stacked(blocks, a):
        return jnp.concatenate([blocks[seqs * a + s] for s in range(seqs)], axis=0)

    def wide(blocks):
        return jnp.concatenate([stacked(blocks, a) for a in range(nx)], axis=1)

    def gain(norm, a):
        return norm[ny * a + y]

    tall = seqs * PART

    def normed(k, h, blocks, norm):
        total = None
        for a in range(nx):
            v = stacked(blocks, a).astype(F32)
            gn[h, :, a * rows : (a + 1) * rows] = (v * gain(norm, a)).astype(BF16)
            part = row_sums(v * v)
            total = part if total is None else total + part
        sq[k, h, y] = total
        return links.share(YA, sq.at[k, h, y])

    def find_inverse(k, h):
        total = sq[k, h, 0]
        for there in range(1, ny):
            total = total + sq[k, h, there]
        inv[k, h] = as_columns(lax.rsqrt(total / width + EPSILON))

    def inverse(k, h, s, n):
        spot = pl.ds(pl.multiple_of(s * PART, PART), PART)
        return widened(inv[k, h, spot, :], n)

    def scatter_y(h, lhs, weights, sent, landed):
        copies = []
        for e in range(nc - 1, -1, -1):
            hh = (hh_h + e) % nc
            part = nn(lhs, weights[hh]).astype(BF16)
            for s in range(seqs):
                sent[h, e, s] = part[s * PART : (s + 1) * PART]
            for p in range(seqs - 1, -1, -1):
                slot = e * seqs + p
                if slot:
                    s = (s_h + p) % seqs
                    copies.append(
                        links.start(
                            sent.at[h, e, s], landed.at[h, slot - 1], {YA: nc * s + hh}
                        )
                    )
        return copies

    def total_y(h, sent, landed):
        total = sent[h, 0, s_h].astype(F32)
        for slot in range(ny - 1):
            total = total + landed[h, slot].astype(F32)
        return total

    def scatter_z(k, h, held, weights, extra=None):
        copies = []
        for e in sorted(range(nx), key=lambda e: (-min(e, nx - e), e)):
            a = (a_r + e) % nx
            spot = pl.ds(pl.multiple_of(a * rows, rows), rows)
            part = None
            for hh in range(nc):
                lhs = jnp.concatenate([held[h, nc * s + hh] for s in range(seqs)], axis=0)
                term = nt(lhs, weights[hh, spot, :])
                part = term if part is None else part + term
            part = part.astype(BF16)
            for s in range(seqs):
                sb_z[k, h, e, s] = part[s * PART : (s + 1) * PART]
            for p in range(seqs):
                slot = e * seqs + p
                if slot == 0:
                    continue
                s = (s_r + p) % seqs
                there = {ZA: seqs * a + s}
                copies.append(
                    links.start(sb_z.at[k, h, e, s], rb_z.at[k, h, slot - 1], there)
                )
                if extra is not None:
                    copies.append(
                        links.start(pz.at[extra, h, s], rb_dot.at[extra, h, slot - 1], there)
                    )
        return copies

    def total_z(k, h):
        total = sb_z[k, h, 0, s_r].astype(F32)
        for slot in range(nz - 1):
            total = total + rb_z[k, h, slot].astype(F32)
        return total

    def chip_sums(k, h):
        for s in range(seqs):
            total = gdot[k, h, nc * s]
            for hh in range(1, nc):
                total = total + gdot[k, h, nc * s + hh]
            pz[k, h, s] = total

    def mean_dot(k, h):
        total = pz[k, h, s_r]
        for slot in range(nz - 1):
            total = total + rb_dot[k, h, slot]
        return widened(as_columns(total / width)[:PART], rows)

    arrived(x_gathered[0])
    sq1 = [normed(0, 0, gx.at[0], norm_a)]
    for h in range(1, CUT):
        arrived(x_gathered[h])
        sq1.append(normed(0, h, gx.at[h], norm_a))
    relay_far("qkv")
    relay("o")
    send_weights("dgu")
    weights_ready("qkv")
    moved = [scatter_y(h, gn[h], wqkv, sb_qkv, rb_qkv) for h in cuts]
    og_gathered = []
    for h in cuts:
        og_moved[h]()
        og_gathered.append(links.share(ZA, gog.at[h, z]))
    bias_here.wait()
    arrived(small)
    relay_far("o")
    weights_ready("o")
    relay("d")
    par = par_all[hh_h]
    scale_key = par[:, 0:head_cols]
    scale_value = par[:, head_cols : 2 * head_cols]
    scale_ffn = par[:, 2 * head_cols : 2 * head_cols + ff_cols]
    for h in cuts:
        arrived(sq1[h])
        find_inverse(0, h)
        arrived(moved[h])
        part = pl.ds(h * PART, PART)
        raw = total_y(h, sb_qkv, rb_qkv) * inverse(0, h, s_h, 3 * head_cols)
        key_pre = raw[:, head_cols : 2 * head_cols]
        value_pre = raw[:, 2 * head_cols :]
        kv_pre[0, part, :] = key_pre
        kv_pre[1, part, :] = value_pre
        qkv_low[0, part, :] = raw[:, :head_cols].astype(BF16)
        qkv_low[1, part, :] = (key_pre * scale_key).astype(BF16)
        qkv_low[2, part, :] = (value_pre * scale_value).astype(BF16)
    lane = lax.broadcasted_iota(jnp.int32, (TOK, TOK), 1)
    real = lane.astype(F32) < len_all[nc * s_h + c]
    halves = [lane < HEAD_DIM, lane >= HEAD_DIM]
    zero = jnp.zeros((TOK, TOK), F32)

    def half_of(pair, half):
        return jnp.where(halves[half], pair.astype(F32), zero).astype(BF16)

    pairs = head_cols // TOK
    for pair in range(pairs):
        cols = slice(pair * TOK, (pair + 1) * TOK)
        q2, k2, v2 = (qkv_low[i, :, cols] for i in range(3))
        parts = []
        for half in range(2):
            head = 2 * pair + half
            scores = nt(half_of(q2, half), k2) + bias_all[hh_h, head]
            scores = jnp.where(real, scores, NEGATIVE)
            exponent = jnp.exp(scores - jnp.max(scores, axis=1, keepdims=True))
            prob = exponent / jnp.sum(exponent, axis=1, keepdims=True)
            probs[head] = prob
            parts.append(nn(prob.astype(BF16), v2))
        context = jnp.where(halves[0], parts[0], parts[1]).astype(BF16)
        for h in cuts:
            gctx[h, y, :, cols] = context[h * PART : (h + 1) * PART]
    ctx_gathered = [links.share(YA, gctx.at[h, y]) for h in cuts]

    root = math.sqrt(2.0 / math.pi)
    out_sums, first, second_norm, hidden_dots = {}, {}, {}, {}
    partial, dgu_gathered, hid_gathered, d_out, df_gathered, dc_moved = {}, {}, {}, {}, {}, {}
    dh_moved, sums = {}, []

    def out_product(h):
        arrived(ctx_gathered[h])
        out_sums[h] = scatter_z(0, h, gctx, wo)

    def first_residual(h):
        arrived(out_sums[h])
        first_sum = gx[h, z].astype(F32) + total_z(0, h)
        fs_r[h] = first_sum
        gfs[h, z] = first_sum.astype(BF16)
        first[h] = links.share(ZA, gfs.at[h, z])

    def hidden_grads():
        relay("gu")
        relay_far("d")
        weights_ready("d")
        for h in cuts:
            arrived(og_gathered[h])
            dh_moved[h] = scatter_y(h, wide(gog.at[h]), wd, sb_dh, rb_dh)
        relay_far("gu")

    def gate_and_up(h):
        if h == 0:
            hidden_grads()
        arrived(first[h])
        second_norm[h] = normed(1, h, gfs.at[h], norm_f)
        if h == 0:
            weights_ready("gu")
        partial[h] = scatter_y(h, gn[h], wgu, sb_gu, rb_gu)

    def hidden_units(h):
        arrived(second_norm[h])
        find_inverse(1, h)
        arrived(dh_moved[h])
        d_hidden = total_y(h, sb_dh, rb_dh)
        arrived(partial[h])
        both = total_y(h, sb_gu, rb_gu) * inverse(1, h, s_h, 2 * ff_cols)
        gate, up = both[:, :ff_cols], both[:, ff_cols:]
        squared = gate * gate
        tanh = jnp.tanh(root * (gate + 0.044715 * gate * squared))
        activated = 0.5 * gate * (1.0 + tanh)
        slope = 0.5 * (1.0 + tanh) + 0.5 * gate * (1.0 - tanh * tanh) * (
            root * (1.0 + (3.0 * 0.044715) * squared)
        )
        product = activated * up
        d_product = d_hidden * scale_ffn
        d_gate = (d_product * up * slope).astype(BF16)
        d_up = (d_product * activated).astype(BF16)
        gdgu[h, y, :, :ff_cols] = d_gate
        gdgu[h, y, :, ff_cols:] = d_up
        dgu_gathered[h] = links.share(YA, gdgu.at[h, y])
        gdot[0, h, y] = row_sums(d_gate.astype(F32) * gate + d_up.astype(F32) * up)
        hidden_dots[h] = links.share(YA, gdot.at[0, h, y])
        ghid[h, y] = (product * scale_ffn).astype(BF16)
        sums.append(jnp.sum(d_hidden * product, axis=0, keepdims=True))
        if h == CUT - 1:
            for i in cuts:
                hid_gathered[i] = links.share(YA, ghid.at[i, y])
            total = sums[0]
            for part in sums[1:]:
                total = total + part
            gv[0, 0, :, 2 * head_cols :] = total

    def second_grad(h):
        arrived(hidden_dots[h])
        chip_sums(0, h)
        arrived(dgu_gathered[h])
        d_out[h] = scatter_z(1, h, gdgu, wgu, 0)

    def first_grad(h):
        inv_second = inverse(1, h, s_r, rows)
        arrived(d_out[h])
        d_first = (
            gog[h, z].astype(F32)
            + inv_second * (total_z(1, h) * gain(norm_f, a_r))
            - fs_r[h] * (inv_second * inv_second * mean_dot(0, h))
        )
        df_r[h] = d_first
        gdf[h, z] = d_first.astype(BF16)
        df_gathered[h] = links.share(ZA, gdf.at[h, z])

    def context_grad(h):
        arrived(df_gathered[h])
        dc_moved[h] = scatter_y(h, wide(gdf.at[h]), wo, sb_dc, rb_dc)

    wave = (
        out_product,
        first_residual,
        gate_and_up,
        hidden_units,
        second_grad,
        first_grad,
        context_grad,
    )
    for step in range(len(wave) + CUT - 1):
        for k, stage in enumerate(wave):
            if 0 <= step - k < CUT:
                stage(step - k)
    ff_moved = []
    for h in cuts:
        arrived(hid_gathered[h])
        ff_moved.append(scatter_z(2, h, ghid, wd))
    d_context = []
    for h in cuts:
        arrived(dc_moved[h])
        d_context.append(total_y(h, sb_dc, rb_dc).astype(BF16))
    d_context = jnp.concatenate(d_context, axis=0)
    for pair in range(pairs):
        cols = slice(pair * TOK, (pair + 1) * TOK)
        q2, k2, v2 = (qkv_low[i, :, cols] for i in range(3))
        dc2 = d_context[:, cols]
        dq, dk, dv = [], [], []
        for half in range(2):
            prob = probs[2 * pair + half]
            d_probs = nt(half_of(dc2, half), v2)
            inner = jnp.sum(prob * d_probs, axis=1, keepdims=True)
            d_scores = prob * (d_probs - inner)
            dq.append(nn(d_scores.astype(BF16), k2))
            dk.append(nn(d_scores.T.astype(BF16), q2))
            dv.append(nn(prob.T.astype(BF16), dc2))
        d_query, d_key, d_value = (jnp.where(halves[0], *two) for two in (dq, dk, dv))
        key2, value2 = kv_pre[0, :, cols], kv_pre[1, :, cols]
        at = pair * TOK
        gv[0, 0, :, at : at + TOK] = jnp.sum(d_key * key2, axis=0, keepdims=True)
        at += head_cols
        gv[0, 0, :, at : at + TOK] = jnp.sum(d_value * value2, axis=0, keepdims=True)
        d_query = d_query.astype(BF16)
        d_key = (d_key * scale_key[:, cols]).astype(BF16)
        d_value = (d_value * scale_value[:, cols]).astype(BF16)
        terms = (
            d_query.astype(F32) * q2.astype(F32)
            + d_key.astype(F32) * key2
            + d_value.astype(F32) * value2
        )
        sums = [row_sums(terms[h * PART : (h + 1) * PART]) for h in cuts]
        dots = sums if pair == 0 else [old + new for old, new in zip(dots, sums)]
        for i, part in enumerate((d_query, d_key, d_value)):
            at = i * head_cols + pair * TOK
            for h in cuts:
                gdqkv[h, y, :, at : at + TOK] = part[h * PART : (h + 1) * PART]
    dqkv_gathered, dot_gathered = [], []
    for h in cuts:
        gdot[1, h, y] = dots[h]
        dot_gathered.append(links.share(YA, gdot.at[1, h, y]))
        dqkv_gathered.append(links.share(YA, gdqkv.at[h, y]))

    gv_c = links.share(CA, gv.at[0, 0], gv.at[0, 1])
    moved = []
    for h in cuts:
        arrived(dot_gathered[h])
        chip_sums(1, h)
        arrived(dqkv_gathered[h])
        moved.append(scatter_z(3, h, gdqkv, wqkv, 1))
        if h == 0:
            arrived(gv_c)
            total = gv[0, 0]
            if nc > 1:
                total = total + gv[0, 1]
            gv[1, y] = total
            gv_y = links.share(YA, gv.at[1, y])
        if h == CUT - 1:
            arrived(gv_y)
            total = gv[1, c]
            for s in range(1, seqs):
                total = total + gv[1, nc * s + c]
            gv[2, x] = total
            gv_x = links.share(XA, gv.at[2, x])
    out_moved = []
    for h in cuts:
        arrived(ff_moved[h])
        tout[0, h] = (fs_r[h] + total_z(2, h)).astype(BF16)
        out_moved.append(swapped(tout.at[0, h], tout.at[2, h]))
    ig_moved = []
    for h in cuts:
        inv_first = inverse(0, h, s_r, rows)
        arrived(moved[h])
        tout[1, h] = (
            df_r[h]
            + inv_first * (total_z(3, h) * gain(norm_a, a_r))
            - gx[h, z].astype(F32) * (inv_first * inv_first * mean_dot(1, h))
        ).astype(BF16)
        ig_moved.append(swapped(tout.at[1, h], tout.at[3, h]))
    arrived(gv_x)
    total = gv[2, 0]
    for there in range(1, nx):
        total = total + gv[2, there]
    gk_ref[...] = total[:, :head_cols]
    gv_ref[...] = total[:, head_cols : 2 * head_cols]
    gf_ref[...] = total[:, 2 * head_cols :]
    for h in cuts:
        part = pl.ds(h * PART, PART)
        out_moved[h]()
        out_ref[part, :] = tout[2, h]
        ig_moved[h]()
        ig_ref[part, :] = tout[3, h]
    for copy in links.sent:
        copy.wait_send()


def publish_kernel(out_in, ig_in, gk_in, gv_in, gf_in, out_ref, ig_ref, gk_ref, gv_ref, gf_ref):
    out_ref[...] = out_in[...]
    ig_ref[...] = ig_in[...]
    gk_ref[...] = gk_in[...]
    gv_ref[...] = gv_in[...]
    gf_ref[...] = gf_in[0]


def on_device(
    sizes,
    hidden_in,
    lengths,
    norm_attn,
    q_weight,
    k_weight,
    v_weight,
    out_weight_t,
    norm_ffn,
    gate_weight,
    up_weight,
    down_weight_t,
    scale_key,
    scale_value,
    scale_ffn,
    out_grad,
    position_bias,
):
    nx, ny, nz, nc = sizes
    seqs = ny // nc
    rows, head_cols = q_weight.shape
    ff_cols = gate_weight.shape[1]
    blocks = nx * ny
    extra = 2 * head_cols + ff_cols
    heads = head_cols // HEAD_DIM
    wide = rows * nx
    vmem, hbm = pl.BlockSpec(memory_space=pltpu.VMEM), pl.BlockSpec(memory_space=pl.ANY)
    smem = pl.BlockSpec(memory_space=pltpu.SMEM)

    def buf(*shape, dtype=BF16):
        return pltpu.VMEM(shape, dtype)

    scratch = [
        buf(nc, wide, 3 * head_cols),
        buf(nc, wide, head_cols),
        buf(nc, wide, 2 * ff_cols),
        buf(nc, wide, ff_cols),
        buf(CUT, nz, PART, rows),
        buf(CUT, nz, PART, rows),
        buf(CUT, seqs * PART, wide),
        buf(2, CUT, ny, 1, TOK, dtype=F32),
        buf(2, CUT, TOK, TOK, dtype=F32),
        buf(nc, heads, TOK, TOK, dtype=F32),
        buf(nc, 1, extra, dtype=F32),
        buf(ny, 1, TOK, dtype=F32),
        buf(CUT, nc, seqs, PART, 3 * head_cols),
        buf(CUT, ny - 1, PART, 3 * head_cols),
        buf(2, TOK, head_cols, dtype=F32),
        buf(3, TOK, head_cols),
        buf(heads, TOK, TOK, dtype=F32),
        buf(CUT, ny, PART, head_cols),
        buf(4, CUT, nx, seqs, PART, rows),
        buf(4, CUT, nz - 1, PART, rows),
        buf(CUT, PART, rows, dtype=F32),
        buf(CUT, nz, PART, rows),
        buf(CUT, nc, seqs, PART, 2 * ff_cols),
        buf(CUT, ny - 1, PART, 2 * ff_cols),
        buf(CUT, nc, seqs, PART, ff_cols),
        buf(CUT, ny - 1, PART, ff_cols),
        buf(CUT, ny, PART, 2 * ff_cols),
        buf(CUT, ny, PART, ff_cols),
        buf(2, CUT, ny, 1, TOK, dtype=F32),
        buf(2, CUT, seqs, 1, TOK, dtype=F32),
        buf(2, CUT, nz - 1, 1, TOK, dtype=F32),
        buf(CUT, PART, rows, dtype=F32),
        buf(CUT, nz, PART, rows),
        buf(CUT, nc, seqs, PART, head_cols),
        buf(CUT, ny - 1, PART, head_cols),
        buf(CUT, ny, PART, 3 * head_cols),
        buf(3, max(nx, ny, 2), 1, extra, dtype=F32),
        buf(4, CUT, PART, rows),
        pltpu.SemaphoreType.DMA((640,)),
        pltpu.SemaphoreType.DMA((640,)),
    ]
    block_out, input_grad, grad_key, grad_value, grad_ffn = pl.pallas_call(
        functools.partial(layer_kernel, sizes),
        out_shape=(
            jax.ShapeDtypeStruct((TOK, rows), BF16),
            jax.ShapeDtypeStruct((TOK, rows), BF16),
            jax.ShapeDtypeStruct((1, head_cols), F32),
            jax.ShapeDtypeStruct((1, head_cols), F32),
            jax.ShapeDtypeStruct((1, ff_cols), F32),
        ),
        in_specs=[hbm] * 10 + [vmem] * 5 + [smem],
        out_specs=(vmem,) * 5,
        scratch_shapes=scratch,
        compiler_params=pltpu.CompilerParams(
            collective_id=0, has_side_effects=True, vmem_limit_bytes=60 * 1024 * 1024
        ),
    )(
        hidden_in,
        out_grad,
        q_weight,
        k_weight,
        v_weight,
        out_weight_t,
        gate_weight,
        up_weight,
        down_weight_t,
        position_bias,
        norm_attn.reshape(blocks, 1, rows),
        norm_ffn.reshape(blocks, 1, rows),
        scale_key[None],
        scale_value[None],
        scale_ffn[None],
        lengths,
    )
    results = pl.pallas_call(
        publish_kernel,
        out_shape=(
            jax.ShapeDtypeStruct((TOK, rows), BF16),
            jax.ShapeDtypeStruct((TOK, rows), BF16),
            jax.ShapeDtypeStruct((1, head_cols), F32),
            jax.ShapeDtypeStruct((1, head_cols), F32),
            jax.ShapeDtypeStruct((ff_cols,), F32),
        ),
        in_specs=[vmem] * 5,
        out_specs=(vmem,) * 5,
    )(block_out, input_grad, grad_key, grad_value, grad_ffn)
    block_out, input_grad, grad_key, grad_value, grad_ffn = results
    return block_out, input_grad, grad_key[0], grad_value[0], grad_ffn


def solution(mesh, sizes=(4, 4, 8, 2)):
    finer = Mesh(mesh.devices.reshape(sizes), AXES)
    dp, mp = (XA, YA), (ZA, CA)
    placed = (
        P(dp, mp),
        P(dp),
        P(),
        P(dp, mp),
        P(dp, mp),
        P(dp, mp),
        P(dp, mp),
        P(),
        P(dp, mp),
        P(dp, mp),
        P(dp, mp),
        P(mp),
        P(mp),
        P(mp),
        P(dp, None),
        P(mp, None, None),
    )
    return jax.shard_map(
        functools.partial(on_device, sizes),
        mesh=finer,
        in_specs=placed,
        out_specs=(P(dp, mp), P(dp, mp), P(mp), P(mp), P(mp)),
        check_vma=False,
    )
```
